32 devices in a mesh: row: 4 (over y, core), col: 8 (over z, x).
Axes of the slice: x: 2, y: 2, z: 4, core: 2. Of those that a mesh axis runs over, the one named last changes fastest.
Arguments:
- templates: float32 [96, 3, 1024], P(('row', 'col')), may hold values from -600 to 600
Outputs:
- similar: float32 [96, 96], P(('row', 'col'))
The draws below stay inside these ranges and needn't reach their ends.
All inputs are finite; a program needn't handle non-finite values.
Results may differ from the reference program's by a relative error of at most 0.0012.
Values may be sent and summed in bfloat16 or wider, within the bound.
A program may use at most 128 MiB of HBM per device.

```python
import math
import jax
import jax.numpy as jnp
from jax import lax

COMP = 3
SAMPLES = 1024
LAGS = 512
NFFT = 1280
NT = 96


def draw_templates(key, part):
    subkeys = jax.random.split(key, 6)
    noise_part = jnp.clip(jax.random.normal(subkeys[0], (NT, COMP, SAMPLES), jnp.float32), -6.0, 6.0)
    weight = jax.random.uniform(subkeys[4], (NT, 1, 1), jnp.float32, 0.0, 1.5)
    scales = jnp.exp(jax.random.uniform(subkeys[5], (NT, COMP, 1), jnp.float32, 0.0, jnp.log(10.0)))
    clusters = jnp.clip(jax.random.normal(subkeys[1], (8, COMP, SAMPLES), jnp.float32), -6.0, 6.0)
    member = jax.random.randint(subkeys[2], (NT,), 0, 8)
    shifts = jax.random.randint(subkeys[3], (NT,), -(LAGS // 4), LAGS // 4 + 1)
    source_idx = (jnp.arange(SAMPLES, dtype=jnp.int32)[None, :] - shifts[:, None]) % SAMPLES
    chosen = clusters[member]
    shifted = jnp.take_along_axis(chosen, jnp.broadcast_to(source_idx[:, None, :], (NT, COMP, SAMPLES)), axis=2)
    return ((weight * shifted + noise_part) * scales).astype(jnp.float32)


def setup_inputs(seed: int = 0) -> dict:
    splits = jax.random.split(jax.random.key(seed), 2)
    templates = draw_templates(jax.random.fold_in(splits[1], 71), 0)
    return {"templates": templates}


def normalize(templates):
    scaling = lax.rsqrt(lax.optimization_barrier(jnp.mean(templates * templates, axis=2, keepdims=True)) + 1e-06) / math.sqrt(templates.shape[2])
    return (templates * scaling).astype(jnp.bfloat16)

def forward_table(samples, transform_len):
    half_len = transform_len // 2
    sample_idx = jnp.arange(samples, dtype=jnp.int32)[:, None]
    slot_idx = jnp.arange(transform_len, dtype=jnp.int32)[None, :]
    freq_idx = jnp.where(slot_idx < half_len, slot_idx, slot_idx - half_len)
    phases = sample_idx * freq_idx % transform_len
    angles = phases.astype(jnp.float32) * (2.0 * math.pi / transform_len)
    nyquist = jnp.where(sample_idx % 2 == 0, 1.0, -1.0)
    basis = jnp.where(slot_idx < half_len, jnp.cos(angles), jnp.where(slot_idx == half_len, nyquist, -jnp.sin(angles)))
    return basis.astype(jnp.bfloat16)

def inverse_table(transform_len, lag_total):
    half_len = transform_len // 2
    slot_idx = jnp.arange(transform_len, dtype=jnp.int32)[:, None]
    lag_idx = jnp.arange(lag_total, dtype=jnp.int32)[None, :] - lag_total // 2
    freq_idx = jnp.where(slot_idx < half_len, slot_idx, slot_idx - half_len)
    phases = freq_idx * lag_idx % transform_len
    angles = phases.astype(jnp.float32) * (2.0 * math.pi / transform_len)
    weight = jnp.where(freq_idx == 0, 1.0, 2.0) / transform_len
    nyquist = jnp.where(lag_idx % 2 == 0, 1.0, -1.0) / transform_len
    basis = jnp.where(slot_idx < half_len, weight * jnp.cos(angles), jnp.where(slot_idx == half_len, nyquist, -weight * jnp.sin(angles)))
    return basis.astype(jnp.bfloat16)

def spectra_of(normed, basis):
    row_total, comps, samples = normed.shape
    flattened = normed.reshape(row_total * comps, samples)
    spectrum = jnp.dot(flattened, basis, preferred_element_type=jnp.float32)
    return spectrum.astype(jnp.bfloat16).reshape(row_total, comps, basis.shape[1])

def pair_einsum(left_part, right_part):
    return jnp.einsum('icf,jcf->ijf', left_part.astype(jnp.float32), right_part.astype(jnp.float32))

def similarity(left_spec, right_spec, inverse):
    half_len = left_spec.shape[2] // 2
    left_real = left_spec[:, :, :half_len]
    left_imag = left_spec[:, :, half_len:]
    right_real = right_spec[:, :, :half_len]
    right_imag = right_spec[:, :, half_len:]
    above_zero = jnp.arange(half_len, dtype=jnp.int32) >= 1
    right_masked = jnp.where(above_zero, right_imag, jnp.zeros_like(right_imag))
    left_masked = jnp.where(above_zero, left_real, jnp.zeros_like(left_real))
    right_turned = jnp.where(above_zero, -right_real, right_imag)
    even_part = pair_einsum(jnp.concatenate([left_real, left_imag], axis=1), jnp.concatenate([right_real, right_masked], axis=1))
    odd_part = pair_einsum(jnp.concatenate([left_masked, left_imag], axis=1), jnp.concatenate([right_imag, right_turned], axis=1))
    cross_spec = jnp.concatenate([even_part, odd_part], axis=2).astype(jnp.bfloat16)
    left_rows = left_spec.shape[0]
    right_rows = right_spec.shape[0]
    lagged = jnp.dot(cross_spec.reshape(left_rows * right_rows, 2 * half_len), inverse, preferred_element_type=jnp.float32)
    return lax.optimization_barrier(jnp.max(lagged, axis=1)).reshape(left_rows, right_rows)

def reference(templates):
    forward = forward_table(SAMPLES, NFFT)
    inverse = inverse_table(NFFT, LAGS)
    spectrum = spectra_of(normalize(templates), forward)
    block_total = math.gcd(NT, 64)
    pieces = spectrum.reshape(block_total, NT // block_total, COMP, NFFT)
    similar = lax.map(lambda row_piece: similarity(row_piece, spectrum, inverse), pieces)
    return similar.reshape(NT, NT)
```

```python
import functools
import math

import jax
import jax.numpy as jnp
from jax import lax
from jax.experimental import pallas as pl
from jax.experimental.pallas import tpu as pltpu
from jax.sharding import PartitionSpec as P

LAGS = 512
LANES = 128
SUBS = 8
CORES = 2
STEP = 32
SEGMENT = 40
MESH = pl.DeviceIdType.MESH


def each(count, step):
    if count <= 16:
        for k in range(count):
            step(k)
    else:
        lax.fori_loop(0, count, lambda k, carry: (step(k), carry)[1], 0)


def when(condition, step):
    pl.when(condition)(step)


def kernel(
    rows,
    cols,
    x_hbm,
    out_ref,
    x_ref,
    stage,
    gathered,
    flat,
    moved,
    waves,
    shifts,
    own_rows,
    other_rows,
    theirs,
    outbox,
    inbox,
    total,
    send_sem,
    recv_sem,
    note_send_sem,
    note_recv_sem,
    near_sem,
):
    n, comps, samples = x_ref.shape
    chunks = samples // LANES
    lines = n * comps * chunks
    tall = rows // CORES
    wide = 2 ** int(math.log2(math.sqrt(cols)))
    deep = cols // wide
    plane = tall * wide
    slots = plane * deep
    group = math.gcd(plane, 4)
    height = waves.shape[2]
    width = total.shape[1]
    blocks = LAGS // STEP
    tiles = chunks + 1
    row = lax.axis_index("row")
    col = lax.axis_index("col")
    my_y, my_core = row // CORES, row % CORES
    my_z, my_x = col // wide, col % wide
    other = 1 - my_core
    mine = my_z * plane + my_y * wide + my_x

    def where_is(slot):
        xy, z = slot % plane, slot // plane
        return xy // wide, xy % wide, z

    def place(slot, core):
        y, x, z = where_is(slot)
        return y * CORES + core, z * wide + x

    def column(slot, core):
        y, x, z = where_is(slot)
        return ((y * CORES + core) * cols + z * wide + x) * n

    by_level = sorted(range(slots), key=lambda s: (sum(where_is(s)), s))

    def chips(step):
        each(slots, lambda k: step(by_level[k] if isinstance(k, int) else k))

    barrier = pltpu.get_barrier_semaphore()

    def greet(slot, core):
        pl.semaphore_signal(barrier, inc=1, device_id=place(slot, core), device_id_type=MESH)

    chips(lambda slot: when(slot > mine, lambda: greet(slot, other)))
    greet(mine, other)

    taken = pltpu.make_async_copy(x_hbm, x_ref, near_sem.at[0])
    taken.start()
    taken.wait()

    for t in range(n):
        x = x_ref[t]
        scale = lax.rsqrt(jnp.mean(x * x, axis=1, keepdims=True) + 1e-06) / math.sqrt(samples)
        rounded = (x * scale).astype(jnp.bfloat16).astype(jnp.float32)
        for q in range(chunks):
            stage[pl.ds(t * comps * chunks + q, comps, stride=chunks), :] = rounded[
                :, q * LANES : (q + 1) * LANES
            ]
    gathered[mine] = stage[:lines].reshape(n * comps, chunks, LANES).astype(jnp.bfloat16)
    pl.semaphore_wait(barrier, mine + 1)

    def block(slot):
        return pltpu.make_async_remote_copy(
            src_ref=gathered.at[mine],
            dst_ref=gathered.at[mine],
            send_sem=send_sem.at[slot],
            recv_sem=recv_sem.at[mine],
            device_id=place(slot, other),
            device_id_type=MESH,
        )

    def arrived(slot):
        pltpu.make_async_remote_copy(
            src_ref=gathered.at[slot],
            dst_ref=gathered.at[slot],
            send_sem=send_sem.at[slot],
            recv_sem=recv_sem.at[slot],
            device_id=place(mine, other),
            device_id_type=MESH,
        ).wait_recv()

    sibling = pltpu.make_async_remote_copy(
        src_ref=gathered.at[mine],
        dst_ref=gathered.at[slots],
        send_sem=near_sem.at[1],
        recv_sem=near_sem.at[2],
        device_id=place(mine, other),
        device_id_type=MESH,
    )

    chips(lambda slot: when(slot < mine, lambda: block(slot).start()))
    sibling.start()

    def shifted_copies(half):
        local = jnp.concatenate(
            [
                stage[pl.ds(half * lines + q, n * comps, stride=chunks), :]
                for q in range(chunks)
            ]
            + [jnp.zeros((n * comps, LANES), jnp.float32)],
            axis=1,
        )
        for c in range(comps):
            parts = []
            for t in range(n):
                line = local[t * comps + c : t * comps + c + 1]
                line = jnp.broadcast_to(line, (SEGMENT, tiles * LANES))
                parts.append(pltpu.roll(line, 0, 1, stride=1, stride_axis=0))
            parts.append(jnp.zeros((LANES - n * SEGMENT, tiles * LANES), jnp.float32))
            stood = jnp.concatenate(parts, axis=0).T.astype(jnp.bfloat16)
            at = slice(half * LANES, (half + 1) * LANES)
            shifts[c * samples : (c + 1) * samples, at] = stood[:samples]
            tail = comps * samples + c * LANES
            shifts[tail : tail + LANES, at] = stood[samples:]

    own_rows[...] = jnp.zeros(own_rows.shape, jnp.float32)
    other_rows[...] = jnp.zeros(other_rows.shape, jnp.float32)
    total[...] = jnp.zeros(total.shape, jnp.float32)
    for b in range(LANES // STEP):
        for c in range(comps):
            waves[b, c, :, : 2 * LANES] = jnp.zeros((height, 2 * LANES), jnp.bfloat16)
            waves[b, c, :, (chunks + 2) * LANES :] = jnp.zeros(
                (height, 2 * LANES), jnp.bfloat16
            )
    shifted_copies(0)
    sibling.wait_recv()
    stage[lines:] = gathered[slots].astype(jnp.float32).reshape(lines, LANES)
    shifted_copies(1)

    def note(g, slot):
        return pltpu.make_async_remote_copy(
            src_ref=outbox.at[g],
            dst_ref=inbox.at[mine],
            send_sem=note_send_sem.at[slot],
            recv_sem=note_recv_sem.at[mine],
            device_id=place(slot, other),
            device_id_type=MESH,
        )

    stride = comps * chunks

    def compare(g, carry):
        first = g * group
        tops = lax.broadcasted_iota(jnp.int32, (height, width), 0)
        lane = lax.broadcasted_iota(jnp.int32, (height, width), 1)
        target = jnp.full((height, width), -1, jnp.int32)
        for k in range(group):
            slot = first + k
            core = jnp.where(slot == mine, my_core, other)
            start = jnp.where(slot >= mine, column(slot, core) - k * n, -slots * n * n)
            here = (tops >= k * n) & (tops < (k + 1) * n)
            target = jnp.where(here, start + tops, target)
        spot = lane == target

        each(group, lambda k: when(first + k > mine, lambda: arrived(first + k)))
        flat[: group * lines] = (
            gathered[pl.ds(first, group)].astype(jnp.float32).reshape(group * lines, LANES)
        )
        for c in range(comps):
            wave = jnp.concatenate(
                [flat[pl.ds(c * chunks + q, height, stride=stride), :] for q in range(chunks)]
                + [jnp.zeros((height, LANES), jnp.float32)],
                axis=1,
            )
            for b in range(LANES // STEP):
                turned = wave if b == 0 else pltpu.roll(wave, tiles * LANES - b * STEP, 1)
                turned = turned.astype(jnp.bfloat16)
                waves[b, c, :, 2 * LANES : (chunks + 2) * LANES] = turned[:, :samples]
                if b:
                    waves[b, c, :, LANES : 2 * LANES] = turned[:, samples:]

        def lined_up(c, at, size):
            parts = []
            for p in range(blocks):
                a, b = p * STEP // LANES, p % (LANES // STEP)
                start = at + a * LANES
                parts.append(waves[b, c, :, start : start + size])
            return jnp.concatenate(parts, axis=0)

        found = jnp.zeros((blocks * height, 2 * LANES), jnp.float32)
        for c in range(comps):
            for at in range(0, samples, 2 * LANES):
                base = c * samples + at
                found = found + jnp.dot(
                    lined_up(c, at, 2 * LANES),
                    shifts[base : base + 2 * LANES],
                    preferred_element_type=jnp.float32,
                )
        for c in range(comps):
            base = comps * samples + c * LANES
            found = found + jnp.dot(
                lined_up(c, samples, LANES),
                shifts[base : base + LANES],
                preferred_element_type=jnp.float32,
            )

        def part(p):
            return found[p * height : (p + 1) * height]

        low, high = part(0), part(blocks - 1)
        middle = part(1)
        for p in range(2, blocks - 1):
            middle = jnp.maximum(middle, part(p))
        ours = jnp.zeros((height, width), jnp.float32)
        place_lane = lax.broadcasted_iota(jnp.int32, (height, LANES), 1)
        note_lane = lane
        for half in range(CORES):
            at = slice(half * LANES, (half + 1) * LANES)
            mid, first_block, last_block = middle[:, at], low[:, at], high[:, at]
            core = my_core if half == 0 else other
            into = own_rows if half == 0 else other_rows
            start = column(mine, core)
            for t in range(n):
                v = place_lane - t * SEGMENT
                inside = (v >= 0) & (v < SEGMENT)
                plain = jnp.maximum(
                    jnp.where(inside, jnp.maximum(mid, first_block), -jnp.inf),
                    jnp.where((v >= 0) & (v < STEP), last_block, -jnp.inf),
                )
                turned = jnp.maximum(
                    jnp.where(inside, mid, -jnp.inf),
                    jnp.maximum(
                        jnp.where((v >= 1) & (v < SEGMENT), first_block, -jnp.inf),
                        jnp.where((v >= 0) & (v <= STEP), last_block, -jnp.inf),
                    ),
                )
                best = jnp.max(plain, axis=1, keepdims=True)
                into[t : t + 1] += jnp.sum(
                    jnp.where(spot, best, 0.0), axis=0, keepdims=True
                )
                best = jnp.max(turned, axis=1, keepdims=True)
                ours = jnp.where(note_lane == start + t, best, ours)
        outbox[g] = ours
        each(group, lambda k: when(first + k > mine, lambda: note(g, first + k).start()))
        return carry

    lax.fori_loop(mine // group, slots // group, compare, 0)

    swap = pltpu.make_async_remote_copy(
        src_ref=other_rows,
        dst_ref=theirs,
        send_sem=near_sem.at[3],
        recv_sem=near_sem.at[4],
        device_id=place(mine, other),
        device_id_type=MESH,
    )
    swap.start()

    def collect(slot):
        pltpu.make_async_remote_copy(
            src_ref=outbox.at[0],
            dst_ref=inbox.at[slot],
            send_sem=note_send_sem.at[slot],
            recv_sem=note_recv_sem.at[slot],
            device_id=place(mine, other),
            device_id_type=MESH,
        ).wait_recv()
        total[...] += inbox[slot]

    chips(lambda slot: when(slot < mine, lambda: collect(slot)))
    moved[...] = pltpu.roll(total[...], (height - mine % group * n) % height, 0)
    swap.wait_recv()
    answer = moved[:n] + own_rows[:n] + theirs[:n]
    out_ref[...] = answer[:, : out_ref.shape[1]]

    chips(lambda slot: when(slot < mine, lambda: block(slot).wait_send()))
    chips(lambda slot: when(slot > mine, lambda: note(0, slot).wait_send()))
    sibling.wait_send()
    swap.wait_send()


def body(templates):
    n, comps, samples = templates.shape
    rows = lax.axis_size("row")
    cols = lax.axis_size("col")
    slots = rows * cols // CORES
    chunks = samples // LANES
    lines = n * comps * chunks
    wide = 2 ** int(math.log2(math.sqrt(cols)))
    group = math.gcd(rows // CORES * wide, 4)
    height = group * n + -(group * n) % 16
    out_width = CORES * slots * n
    width = out_width + -out_width % LANES
    tiles = chunks + 1
    return pl.pallas_call(
        functools.partial(kernel, rows, cols),
        out_shape=pltpu.VMEM((n, out_width), jnp.float32),
        in_specs=[pl.BlockSpec(memory_space=pltpu.HBM)],
        out_specs=pl.BlockSpec(memory_space=pltpu.VMEM),
        scratch_shapes=[
            pltpu.VMEM(templates.shape, jnp.float32),
            pltpu.VMEM((CORES * lines, LANES), jnp.float32),
            pltpu.VMEM((slots + 1, n * comps, chunks, LANES), jnp.bfloat16),
            pltpu.VMEM((height * comps * chunks, LANES), jnp.float32),
            pltpu.VMEM((height, width), jnp.float32),
            pltpu.VMEM((LANES // STEP, comps, height, samples + 4 * LANES), jnp.bfloat16),
            pltpu.VMEM((comps * tiles * LANES, CORES * LANES), jnp.bfloat16),
            pltpu.VMEM((SUBS, width), jnp.float32),
            pltpu.VMEM((SUBS, width), jnp.float32),
            pltpu.VMEM((SUBS, width), jnp.float32),
            pltpu.VMEM((slots // group, height, width), jnp.float32),
            pltpu.VMEM((slots, height, width), jnp.float32),
            pltpu.VMEM((height, width), jnp.float32),
            pltpu.SemaphoreType.DMA((slots,)),
            pltpu.SemaphoreType.DMA((slots,)),
            pltpu.SemaphoreType.DMA((slots,)),
            pltpu.SemaphoreType.DMA((slots,)),
            pltpu.SemaphoreType.DMA((5,)),
        ],
        compiler_params=pltpu.CompilerParams(collective_id=0, has_side_effects=True),
    )(templates)


def solution(mesh):
    placed = (P(("row", "col"), None, None),)
    return jax.shard_map(
        body, mesh=mesh, in_specs=placed, out_specs=P(("row", "col"), None), check_vma=False
    )
```

```python
import functools
import math

import jax
import jax.numpy as jnp
from jax import lax
from jax.experimental import pallas as pl
from jax.experimental.pallas import tpu as pltpu
from jax.sharding import PartitionSpec as P

LAGS = 512
LANES = 128
SUBS = 8
CORES = 2
STEP = 16
MESH = pl.DeviceIdType.MESH


def each(count, step):
    if count <= 16:
        for k in range(count):
            step(k)
    else:
        lax.fori_loop(0, count, lambda k, carry: (step(k), carry)[1], 0)


def when(condition, step):
    pl.when(condition)(step)


def kernel(
    rows,
    cols,
    x_hbm,
    out_ref,
    x_ref,
    stage,
    beside,
    column_blocks,
    lines_ref,
    flat,
    waves,
    shifts,
    answers,
    turned_rows,
    from_plane,
    from_column,
    total,
    block_sem,
    column_sem,
    plane_sem,
    answer_sem,
    turned_sem,
    from_plane_sem,
    from_column_sem,
    table_sem,
):
    n, comps, samples = x_ref.shape
    chunks = samples // LANES
    series = n * comps
    lines = series * chunks
    tall = rows // CORES
    wide = 2 ** int(math.log2(math.sqrt(cols)))
    deep = cols // wide
    plane = tall * wide
    width = total.shape[1]
    blocks = LAGS // STEP
    phases = LANES // STEP
    tiles = chunks + 1
    row = lax.axis_index("row")
    col = lax.axis_index("col")
    my_y, my_core = row // CORES, row % CORES
    my_z, my_x = col // wide, col % wide
    my_xy = my_y * wide + my_x
    other = 1 - my_core

    def place(xy, z, core):
        return (xy // wide) * CORES + core, z * wide + xy % wide

    def column(xy, z, core):
        return (((xy // wide) * CORES + core) * cols + z * wide + xy % wide) * n

    def mates(step):
        each(plane, lambda xy: when(xy != my_xy, lambda: step(xy)))

    def below(step):
        for z in range(deep - 1):
            for core in range(CORES):
                when(z < my_z, lambda: step(z, core))

    def above(step):
        for z in range(1, deep):
            for core in range(CORES):
                when(z > my_z, lambda: step(z, core))

    barrier = pltpu.get_barrier_semaphore()

    def greet(xy, z, core):
        pl.semaphore_signal(barrier, inc=1, device_id=place(xy, z, core), device_id_type=MESH)

    taken = pltpu.make_async_copy(x_hbm, x_ref, table_sem.at[0])
    taken.start()
    mates(lambda xy: greet(xy, my_z, other))
    above(lambda z, core: greet(my_xy, z, core))
    greet(my_xy, my_z, other)
    taken.wait()

    for t in range(n):
        x = x_ref[t]
        scale = lax.rsqrt(jnp.mean(x * x, axis=1, keepdims=True) + 1e-06) / math.sqrt(samples)
        rounded = (x * scale).astype(jnp.bfloat16).astype(jnp.float32)
        for q in range(chunks):
            stage[pl.ds(t * comps * chunks + q, comps, stride=chunks), :] = rounded[
                :, q * LANES : (q + 1) * LANES
            ]
    column_blocks[my_z, my_core] = (
        stage[...].reshape(series, chunks, LANES).astype(jnp.bfloat16)
    )
    pl.semaphore_wait(barrier, CORES * my_z + plane)

    mine = column_blocks.at[my_z, my_core]

    def to_column(z, core):
        return pltpu.make_async_remote_copy(
            src_ref=mine,
            dst_ref=mine,
            send_sem=block_sem.at[z * CORES + core],
            recv_sem=column_sem.at[my_z * CORES + my_core],
            device_id=place(my_xy, z, core),
            device_id_type=MESH,
        )

    def to_mate(xy):
        return pltpu.make_async_remote_copy(
            src_ref=mine,
            dst_ref=beside.at[my_xy],
            send_sem=block_sem.at[deep * CORES + xy],
            recv_sem=plane_sem.at[my_xy],
            device_id=place(xy, my_z, other),
            device_id_type=MESH,
        )

    def from_above(z, core):
        block = column_blocks.at[z, core]
        return pltpu.make_async_remote_copy(
            src_ref=block,
            dst_ref=block,
            send_sem=block_sem.at[z * CORES + core],
            recv_sem=column_sem.at[z * CORES + core],
            device_id=place(my_xy, my_z, other),
            device_id_type=MESH,
        )

    def from_mate(xy):
        return pltpu.make_async_remote_copy(
            src_ref=mine,
            dst_ref=beside.at[xy],
            send_sem=block_sem.at[deep * CORES + xy],
            recv_sem=plane_sem.at[xy],
            device_id=place(xy, my_z, other),
            device_id_type=MESH,
        )

    below(lambda z, core: to_column(z, core).start())
    mates(lambda xy: to_mate(xy).start())
    to_column(my_z, other).start()

    for m in range(phases // 2):
        for c in range(comps):
            waves[m, c, :, :LANES] = jnp.zeros((2 * SUBS, LANES), jnp.bfloat16)
            waves[m, c, :, (chunks + 2) * LANES :] = jnp.zeros(
                (2 * SUBS, 3 * LANES), jnp.bfloat16
            )
    answers[...] = jnp.zeros(answers.shape, jnp.float32)

    def settle(xy):
        when(xy != my_xy, lambda: from_mate(xy).wait_recv())
        block = beside[xy].astype(jnp.float32).reshape(lines, LANES)
        block = jnp.where(jnp.full((lines, LANES), xy) == my_xy, stage[...], block)
        lines_ref[pl.ds(pl.multiple_of(xy * lines, SUBS), lines), :] = block

    each(plane, settle)
    local = jnp.concatenate(
        [lines_ref[pl.ds(q, plane * series, stride=chunks), :] for q in range(chunks)]
        + [jnp.zeros((plane * series, LANES), jnp.float32)],
        axis=1,
    )
    segments = LANES // STEP
    for g in range(shifts.shape[1] // LANES):
        for c in range(comps):
            parts = []
            for i in range(g * segments, (g + 1) * segments):
                if i < plane * n:
                    line = local[i * comps + c : i * comps + c + 1]
                    line = jnp.broadcast_to(line, (STEP, tiles * LANES))
                    parts.append(pltpu.roll(line, 0, 1, stride=1, stride_axis=0))
                else:
                    parts.append(jnp.zeros((STEP, tiles * LANES), jnp.float32))
            stood = jnp.concatenate(parts, axis=0).T.astype(jnp.bfloat16)
            at = slice(g * LANES, (g + 1) * LANES)
            shifts[c * samples : (c + 1) * samples, at] = stood[:samples]
            tail = comps * samples + c * LANES
            shifts[tail : tail + LANES, at] = stood[samples:]

    def answer(xy):
        return pltpu.make_async_remote_copy(
            src_ref=answers.at[0, xy],
            dst_ref=from_plane.at[my_xy],
            send_sem=answer_sem.at[xy],
            recv_sem=from_plane_sem.at[my_xy],
            device_id=place(xy, my_z, other),
            device_id_type=MESH,
        )

    def give_back(z, core):
        return pltpu.make_async_remote_copy(
            src_ref=turned_rows.at[z],
            dst_ref=from_column.at[my_z, my_core],
            send_sem=turned_sem.at[z * CORES + core],
            recv_sem=from_column_sem.at[my_z * CORES + my_core],
            device_id=place(my_xy, z, core),
            device_id_type=MESH,
        )

    lane = lax.broadcasted_iota(jnp.int32, (SUBS, width), 1)
    tops = lax.broadcasted_iota(jnp.int32, (SUBS, width), 0)
    place_lane = lax.broadcasted_iota(jnp.int32, (SUBS, 2 * LANES), 1)
    seat = place_lane % STEP
    stride = comps * chunks

    def compare(k, carry):
        last = k == deep - my_z
        z = jnp.where(last, my_z, my_z + k)
        target = jnp.full((SUBS, width), -1, jnp.int32)
        for core in range(CORES):
            here = (tops >= core * n) & (tops < (core + 1) * n)
            target = jnp.where(here, column(my_xy, z, core) - core * n + tops, target)
        spot = lane == jnp.where(last, -1, target)
        spare = jnp.where(last, 1, 0)

        when(last & (my_z < deep - 1), lambda: mates(lambda xy: answer(xy).start()))
        for core in range(CORES):
            when((z > my_z) | (core != my_core), lambda: from_above(z, core).wait_recv())
        flat[: CORES * lines] = (
            column_blocks[z].astype(jnp.float32).reshape(CORES * lines, LANES)
        )
        for c in range(comps):
            wave = jnp.concatenate(
                [flat[pl.ds(c * chunks + q, SUBS, stride=stride), :] for q in range(chunks)]
                + [jnp.zeros((SUBS, LANES), jnp.float32)],
                axis=1,
            )
            for m in range(phases // 2):
                pair = [
                    wave if b == 0 else pltpu.roll(wave, tiles * LANES - b * STEP, 1)
                    for b in (2 * m, 2 * m + 1)
                ]
                pair = jnp.concatenate(pair, axis=0).astype(jnp.bfloat16)
                waves[m, c, :, 2 * LANES : (chunks + 2) * LANES] = pair[:, :samples]
                waves[m, c, :, LANES : 2 * LANES] = pair[:, samples:]

        def lined_up(c, at, size):
            parts = []
            for p in range(0, blocks + 2, 2):
                start = at + p // phases * LANES
                parts.append(waves[p % phases // 2, c, :, start : start + size])
            return jnp.concatenate(parts, axis=0)

        turned = jnp.zeros((SUBS, width), jnp.float32)
        for g in range(shifts.shape[1] // (2 * LANES)):
            at = slice(2 * g * LANES, 2 * (g + 1) * LANES)
            found = jnp.zeros(((blocks + 2) * SUBS, 2 * LANES), jnp.float32)
            for c in range(comps):
                for start in range(0, samples, 2 * LANES):
                    base = c * samples + start
                    found = found + jnp.dot(
                        lined_up(c, start, 2 * LANES),
                        shifts[base : base + 2 * LANES, at],
                        preferred_element_type=jnp.float32,
                    )
            for c in range(comps):
                base = comps * samples + c * LANES
                found = found + jnp.dot(
                    lined_up(c, samples, LANES),
                    shifts[base : base + LANES, at],
                    preferred_element_type=jnp.float32,
                )

            def part(p):
                return found[p * SUBS : (p + 1) * SUBS]

            middle = part(1)
            for p in range(2, blocks):
                middle = jnp.maximum(middle, part(p))
            plain = jnp.maximum(middle, part(0))
            swapped = jnp.maximum(middle, jnp.where(seat == 0, part(blocks), part(0)))
            for s in range(2 * segments):
                i = g * 2 * segments + s
                if i >= plane * n:
                    break
                xy, t = i // n, i % n
                part_at = slice(s // segments * LANES, (s // segments + 1) * LANES)
                v = place_lane[:, :LANES] - s % segments * STEP
                inside = (v >= 0) & (v < STEP)
                best = jnp.max(
                    jnp.where(inside, plain[:, part_at], -jnp.inf), axis=1, keepdims=True
                )
                answers[spare, xy, t : t + 1] += jnp.sum(
                    jnp.where(spot, best, 0.0), axis=0, keepdims=True
                )
                best = jnp.max(
                    jnp.where(inside, swapped[:, part_at], -jnp.inf), axis=1, keepdims=True
                )
                core = jnp.where(my_xy == xy, my_core, other)
                turned = jnp.where(lane == column(xy, my_z, core) + t, best, turned)
        turned_rows[z] = turned
        for core in range(CORES):
            when((z > my_z) | (core != my_core), lambda: give_back(z, core).start())
        return carry

    lax.fori_loop(1, deep - my_z + 1, compare, 0)

    total[...] = turned_rows[my_z]

    def collect(z, core):
        pltpu.make_async_remote_copy(
            src_ref=turned_rows.at[0],
            dst_ref=from_column.at[z, core],
            send_sem=turned_sem.at[z * CORES + core],
            recv_sem=from_column_sem.at[z * CORES + core],
            device_id=place(my_xy, my_z, other),
            device_id_type=MESH,
        ).wait_recv()
        total[...] += from_column[z, core]

    for z in range(deep):
        for core in range(CORES):
            when((z < my_z) | ((z == my_z) & (core != my_core)), lambda: collect(z, core))
    total[...] = pltpu.roll(total[...], (SUBS - my_core * n) % SUBS, 0)
    total[...] += answers[0, my_xy]

    def hear(xy):
        pltpu.make_async_remote_copy(
            src_ref=answers.at[0, xy],
            dst_ref=from_plane.at[xy],
            send_sem=answer_sem.at[xy],
            recv_sem=from_plane_sem.at[xy],
            device_id=place(xy, my_z, other),
            device_id_type=MESH,
        ).wait_recv()
        total[...] += from_plane[xy]

    when(my_z < deep - 1, lambda: mates(hear))
    out_ref[...] = total[:n, : out_ref.shape[1]]

    below(lambda z, core: to_column(z, core).wait_send())
    mates(lambda xy: to_mate(xy).wait_send())
    to_column(my_z, other).wait_send()
    when(my_z < deep - 1, lambda: mates(lambda xy: answer(xy).wait_send()))
    above(lambda z, core: give_back(z, core).wait_send())
    give_back(my_z, other).wait_send()


def body(templates):
    n, comps, samples = templates.shape
    rows = lax.axis_size("row")
    cols = lax.axis_size("col")
    chunks = samples // LANES
    series = n * comps
    lines = series * chunks
    wide = 2 ** int(math.log2(math.sqrt(cols)))
    deep = cols // wide
    plane = rows // CORES * wide
    out_width = rows * cols * n
    width = out_width + -out_width % LANES
    tiles = chunks + 1
    spread = plane * n * STEP
    spread += -spread % (2 * LANES)
    dma = pltpu.SemaphoreType.DMA
    return pl.pallas_call(
        functools.partial(kernel, rows, cols),
        out_shape=pltpu.VMEM((n, out_width), jnp.float32),
        in_specs=[pl.BlockSpec(memory_space=pltpu.HBM)],
        out_specs=pl.BlockSpec(memory_space=pltpu.VMEM),
        scratch_shapes=[
            pltpu.VMEM(templates.shape, jnp.float32),
            pltpu.VMEM((lines, LANES), jnp.float32),
            pltpu.VMEM((plane, series, chunks, LANES), jnp.bfloat16),
            pltpu.VMEM((deep, CORES, series, chunks, LANES), jnp.bfloat16),
            pltpu.VMEM((plane * lines, LANES), jnp.float32),
            pltpu.VMEM((SUBS * comps * chunks, LANES), jnp.float32),
            pltpu.VMEM(
                (LANES // STEP // 2, comps, 2 * SUBS, samples + 5 * LANES), jnp.bfloat16
            ),
            pltpu.VMEM((comps * tiles * LANES, spread), jnp.bfloat16),
            pltpu.VMEM((2, plane, SUBS, width), jnp.float32),
            pltpu.VMEM((deep, SUBS, width), jnp.float32),
            pltpu.VMEM((plane, SUBS, width), jnp.float32),
            pltpu.VMEM((deep, CORES, SUBS, width), jnp.float32),
            pltpu.VMEM((SUBS, width), jnp.float32),
            dma((deep * CORES + plane,)),
            dma((deep * CORES,)),
            dma((plane,)),
            dma((plane,)),
            dma((deep * CORES,)),
            dma((plane,)),
            dma((deep * CORES,)),
            dma((1,)),
        ],
        compiler_params=pltpu.CompilerParams(collective_id=0, has_side_effects=True),
    )(templates)


def solution(mesh):
    placed = (P(("row", "col"), None, None),)
    return jax.shard_map(
        body, mesh=mesh, in_specs=placed, out_specs=P(("row", "col"), None), check_vma=False
    )
```

```python
import functools
import math

import jax
import jax.numpy as jnp
from jax import lax
from jax.experimental import pallas as pl
from jax.experimental.pallas import tpu as pltpu
from jax.sharding import PartitionSpec as P

LAGS = 512
LANES = 128
SUBS = 8
CORES = 2
STEP = 16
MESH = pl.DeviceIdType.MESH


def each(count, step):
    if count <= 16:
        for k in range(count):
            step(k)
    else:
        lax.fori_loop(0, count, lambda k, carry: (step(k), carry)[1], 0)


def when(condition, step):
    pl.when(condition)(step)


def kernel(
    rows,
    cols,
    x_hbm,
    out_ref,
    x_ref,
    stage,
    beside,
    column_blocks,
    lines_ref,
    flat,
    waves,
    shifts,
    answers,
    turned_rows,
    from_plane,
    from_column,
    total,
    block_sem,
    column_send_sem,
    column_sem,
    plane_sem,
    answer_sem,
    turned_sem,
    from_plane_sem,
    from_column_sem,
    table_sem,
):
    n, comps, samples = x_ref.shape
    chunks = samples // LANES
    series = n * comps
    lines = series * chunks
    tall = rows // CORES
    wide = 2 ** int(math.log2(math.sqrt(cols)))
    deep = cols // wide
    plane = tall * wide
    width = total.shape[1]
    blocks = LAGS // STEP
    phases = LANES // STEP
    tiles = chunks + 1
    row = lax.axis_index("row")
    col = lax.axis_index("col")
    my_y, my_core = row // CORES, row % CORES
    my_z, my_x = col // wide, col % wide
    my_xy = my_y * wide + my_x
    other = 1 - my_core

    def place(xy, z, core):
        return (xy // wide) * CORES + core, z * wide + xy % wide

    def column(xy, z, core):
        return (((xy // wide) * CORES + core) * cols + z * wide + xy % wide) * n

    def mate(k):
        if plane & (plane - 1):
            return (my_xy + k) % plane
        found, bit = 0, 1
        while bit < plane:
            found, bit = found + (my_xy // bit + k // bit) % 2 * bit, bit * 2
        return found

    def mates(step):
        each(plane - 1, lambda k: step(mate(k + 1)))

    def below(step):
        for z in range(deep - 1):
            for core in range(CORES):
                when(z < my_z, lambda: step(z, core))

    def above(step):
        for z in range(1, deep):
            for core in range(CORES):
                when(z > my_z, lambda: step(z, core))

    barrier = pltpu.get_barrier_semaphore()

    def greet(xy, z, core):
        pl.semaphore_signal(barrier, inc=1, device_id=place(xy, z, core), device_id_type=MESH)

    taken = pltpu.make_async_copy(x_hbm, x_ref, table_sem.at[0])
    taken.start()
    mates(lambda xy: greet(xy, my_z, other))
    above(lambda z, core: greet(my_xy, z, core))
    greet(my_xy, my_z, other)
    taken.wait()

    for t in range(n):
        x = x_ref[t]
        scale = lax.rsqrt(jnp.mean(x * x, axis=1, keepdims=True) + 1e-06) / math.sqrt(samples)
        rounded = (x * scale).astype(jnp.bfloat16).astype(jnp.float32)
        for q in range(chunks):
            stage[pl.ds(t * chunks + q, comps, stride=n * chunks), :] = rounded[
                :, q * LANES : (q + 1) * LANES
            ]
    column_blocks[my_z, my_core] = (
        stage[...].reshape(comps, n, chunks, LANES).astype(jnp.bfloat16)
    )
    pl.semaphore_wait(barrier, CORES * my_z + plane)

    mine = column_blocks.at[my_z, my_core]

    def to_column(z, core):
        return pltpu.make_async_remote_copy(
            src_ref=mine,
            dst_ref=mine,
            send_sem=column_send_sem.at[z * CORES + core],
            recv_sem=column_sem.at[my_z * CORES + my_core],
            device_id=place(my_xy, z, core),
            device_id_type=MESH,
        )

    def to_mate(xy):
        return pltpu.make_async_remote_copy(
            src_ref=mine,
            dst_ref=beside.at[my_xy],
            send_sem=block_sem.at[xy],
            recv_sem=plane_sem.at[my_xy],
            device_id=place(xy, my_z, other),
            device_id_type=MESH,
        )

    def from_above(z, core):
        block = column_blocks.at[z, core]
        return pltpu.make_async_remote_copy(
            src_ref=block,
            dst_ref=block,
            send_sem=column_send_sem.at[core],
            recv_sem=column_sem.at[z * CORES + core],
            device_id=place(my_xy, my_z, other),
            device_id_type=MESH,
        )

    def from_mate(xy):
        return pltpu.make_async_remote_copy(
            src_ref=mine,
            dst_ref=beside.at[xy],
            send_sem=block_sem.at[xy],
            recv_sem=plane_sem.at[xy],
            device_id=place(xy, my_z, other),
            device_id_type=MESH,
        )

    def send_down(z):
        to_column(z, my_core).start()
        to_column(z, other).start()

    when(my_z > 0, lambda: send_down(0))
    mates(lambda xy: to_mate(xy).start())
    to_column(my_z, other).start()
    def gone(z):
        for core in range(CORES):
            to_column(z, core).wait_send()

    def send_next(z):
        gone(z - 1)
        send_down(z)


    for m in range(phases // 2):
        for c in range(comps):
            waves[m, c, :, :LANES] = jnp.zeros((2 * SUBS, LANES), jnp.bfloat16)
            waves[m, c, :, (chunks + 2) * LANES :] = jnp.zeros(
                (2 * SUBS, 3 * LANES), jnp.bfloat16
            )
    answers[...] = jnp.zeros(answers.shape, jnp.float32)

    def settle(k):
        if k == 0:
            block = stage[...]
        else:
            from_mate(mate(k)).wait_recv()
            block = beside[mate(k)].astype(jnp.float32).reshape(lines, LANES)
        lines_ref[k * lines : (k + 1) * lines, :] = block

    segments = LANES // STEP
    seats_of = segments // 2

    def stand(g):
        held = range(2 * g, min(2 * g + 2, plane))
        for k in held:
            settle(k)
        local = jnp.concatenate(
            [
                lines_ref[pl.ds(2 * g * lines + q, len(held) * series, stride=chunks), :]
                for q in range(chunks)
            ]
            + [jnp.zeros((len(held) * series, LANES), jnp.float32)],
            axis=1,
        )
        for c in range(comps):
            parts = []
            for s in range(segments):
                k, t = s // seats_of, s % seats_of
                if k < len(held) and t < n:
                    r = k * series + c * n + t
                    line = jnp.broadcast_to(local[r : r + 1], (STEP, tiles * LANES))
                    line = pltpu.roll(line, 0, 1, stride=1, stride_axis=0)
                else:
                    line = jnp.zeros((STEP, tiles * LANES), jnp.float32)
                parts.append(line.astype(jnp.bfloat16))
            stood = jnp.concatenate(parts, axis=0).T
            at = slice(g * LANES, (g + 1) * LANES)
            shifts[c * samples : (c + 1) * samples, at] = stood[:samples]
            tail = comps * samples + c * LANES
            shifts[tail : tail + LANES, at] = stood[samples:]

    for z in range(1, deep - 1):
        when(z < my_z, lambda: send_next(z))
    for g in range((plane + 1) // 2):
        stand(g)

    def answer(k):
        return pltpu.make_async_remote_copy(
            src_ref=answers.at[k],
            dst_ref=from_plane.at[my_xy],
            send_sem=answer_sem.at[k],
            recv_sem=from_plane_sem.at[my_xy],
            device_id=place(mate(k), my_z, other),
            device_id_type=MESH,
        )

    def give_back(z, core):
        return pltpu.make_async_remote_copy(
            src_ref=turned_rows.at[z],
            dst_ref=from_column.at[my_z, my_core],
            send_sem=turned_sem.at[z * CORES + core],
            recv_sem=from_column_sem.at[my_z * CORES + my_core],
            device_id=place(my_xy, z, core),
            device_id_type=MESH,
        )

    lane = lax.broadcasted_iota(jnp.int32, (SUBS, width), 1)
    tops = lax.broadcasted_iota(jnp.int32, (SUBS, width), 0)
    place_lane = lax.broadcasted_iota(jnp.int32, (SUBS, 2 * LANES), 1)
    seat = place_lane % STEP

    def compare(z, own):
        target = jnp.full((SUBS, width), -1, jnp.int32)
        for core in range(CORES):
            here = (tops >= core * n) & (tops < (core + 1) * n)
            target = jnp.where(here, column(my_xy, z, core) - core * n + tops, target)
        spot = lane == target

        def prepare(c):
            flat[c, : CORES * n * chunks] = (
                column_blocks[z, :, c].astype(jnp.float32).reshape(CORES * n * chunks, LANES)
            )
            wave = jnp.concatenate(
                [flat[c, pl.ds(q, SUBS, stride=chunks), :] for q in range(chunks)]
                + [jnp.zeros((SUBS, LANES), jnp.float32)],
                axis=1,
            )
            for m in range(phases // 2):
                pair = [
                    wave if b == 0 else pltpu.roll(wave, tiles * LANES - b * STEP, 1)
                    for b in (2 * m, 2 * m + 1)
                ]
                pair = jnp.concatenate(pair, axis=0).astype(jnp.bfloat16)
                waves[m, c, :, 2 * LANES : (chunks + 2) * LANES] = pair[:, :samples]
                waves[m, c, :, LANES : 2 * LANES] = pair[:, samples:]

        def lined_up(c, at, size):
            parts = []
            for p in range(0, blocks + 2, 2):
                start = at + p // phases * LANES
                parts.append(waves[p % phases // 2, c, :, start : start + size])
            return jnp.concatenate(parts, axis=0)

        def products(g):
            at = slice(2 * g * LANES, 2 * (g + 1) * LANES)
            found = jnp.zeros(((blocks + 2) * SUBS, 2 * LANES), jnp.float32)
            for c in range(comps):
                for start in range(0, samples, 2 * LANES):
                    base = c * samples + start
                    found = found + jnp.dot(
                        lined_up(c, start, 2 * LANES),
                        shifts[base : base + 2 * LANES, at],
                        preferred_element_type=jnp.float32,
                    )
            for c in range(comps):
                base = comps * samples + c * LANES
                found = found + jnp.dot(
                    lined_up(c, samples, LANES),
                    shifts[base : base + LANES, at],
                    preferred_element_type=jnp.float32,
                )
            return found

        wholes = shifts.shape[1] // (2 * LANES)
        if own:
            from_above(z, other).wait_recv()
        else:
            for core in range(CORES):
                from_above(z, core).wait_recv()
        for c in range(comps):
            prepare(c)

        turned = jnp.zeros((SUBS, width), jnp.float32)
        parts = []
        for g in range(wholes):
            found = products(g)

            def part(p):
                return found[p * SUBS : (p + 1) * SUBS]

            middle = part(1)
            for p in range(2, blocks):
                middle = jnp.maximum(middle, part(p))
            plain = jnp.maximum(middle, part(0))
            swapped = jnp.maximum(middle, jnp.where(seat == 0, part(blocks), part(0)))
            parts.append(swapped)
            for k, t, part_at, inside in seats(g):
                if own:
                    break
                best = jnp.max(
                    jnp.where(inside, plain[:, part_at], -jnp.inf), axis=1, keepdims=True
                )
                answers[k, t : t + 1] += jnp.sum(
                    jnp.where(spot, best, 0.0), axis=0, keepdims=True
                )
        if not own:
            when(z == deep - 1, lambda: each(plane - 1, lambda k: answer(k + 1).start()))
        for g in range(wholes):
            for k, t, part_at, inside in seats(g):
                best = jnp.max(
                    jnp.where(inside, parts[g][:, part_at], -jnp.inf), axis=1, keepdims=True
                )
                core = other if k else my_core
                turned = jnp.where(lane == column(mate(k), my_z, core) + t, best, turned)
        turned_rows[z] = turned
        for core in range(CORES):
            if own:
                when(core != my_core, lambda: give_back(z, core).start())
            else:
                give_back(z, core).start()

    def seats(g):
        for s in range(2 * segments):
            k, t = g * 2 * segments // seats_of + s // seats_of, s % seats_of
            if k < plane and t < n:
                v = place_lane[:, :LANES] - s % segments * STEP
                part_at = slice(s // segments * LANES, (s // segments + 1) * LANES)
                yield k, t, part_at, (v >= 0) & (v < STEP)

    lax.fori_loop(my_z + 1, deep, lambda z, carry: (compare(z, False), carry)[1], 0)
    compare(my_z, True)

    total[...] = turned_rows[my_z]

    def collect(z, core):
        pltpu.make_async_remote_copy(
            src_ref=turned_rows.at[0],
            dst_ref=from_column.at[z, core],
            send_sem=turned_sem.at[z * CORES + core],
            recv_sem=from_column_sem.at[z * CORES + core],
            device_id=place(my_xy, my_z, other),
            device_id_type=MESH,
        ).wait_recv()
        total[...] += from_column[z, core]

    for z in range(deep):
        for core in range(CORES):
            when((z < my_z) | ((z == my_z) & (core != my_core)), lambda: collect(z, core))
    total[...] = pltpu.roll(total[...], (SUBS - my_core * n) % SUBS, 0)
    total[...] += answers[0]

    def hear(xy):
        pltpu.make_async_remote_copy(
            src_ref=answers.at[0],
            dst_ref=from_plane.at[xy],
            send_sem=answer_sem.at[0],
            recv_sem=from_plane_sem.at[xy],
            device_id=place(xy, my_z, other),
            device_id_type=MESH,
        ).wait_recv()
        total[...] += from_plane[xy]

    when(my_z < deep - 1, lambda: mates(hear))
    out_ref[...] = total[:n, : out_ref.shape[1]]

    when(my_z > 0, lambda: gone(my_z - 1))
    to_column(my_z, other).wait_send()
    mates(lambda xy: to_mate(xy).wait_send())
    when(my_z < deep - 1, lambda: each(plane - 1, lambda k: answer(k + 1).wait_send()))
    above(lambda z, core: give_back(z, core).wait_send())
    give_back(my_z, other).wait_send()


def body(templates):
    n, comps, samples = templates.shape
    rows = lax.axis_size("row")
    cols = lax.axis_size("col")
    chunks = samples // LANES
    series = n * comps
    lines = series * chunks
    wide = 2 ** int(math.log2(math.sqrt(cols)))
    deep = cols // wide
    plane = rows // CORES * wide
    out_width = rows * cols * n
    width = out_width + -out_width % LANES
    tiles = chunks + 1
    spread = plane * LANES // 2
    spread += -spread % (2 * LANES)
    dma = pltpu.SemaphoreType.DMA
    return pl.pallas_call(
        functools.partial(kernel, rows, cols),
        out_shape=pltpu.VMEM((n, out_width), jnp.float32),
        in_specs=[pl.BlockSpec(memory_space=pltpu.HBM)],
        out_specs=pl.BlockSpec(memory_space=pltpu.VMEM),
        scratch_shapes=[
            pltpu.VMEM(templates.shape, jnp.float32),
            pltpu.VMEM((lines, LANES), jnp.float32),
            pltpu.VMEM((plane, comps, n, chunks, LANES), jnp.bfloat16),
            pltpu.VMEM((deep, CORES, comps, n, chunks, LANES), jnp.bfloat16),
            pltpu.VMEM((plane * lines, LANES), jnp.float32),
            pltpu.VMEM((comps, SUBS * chunks, LANES), jnp.float32),
            pltpu.VMEM(
                (LANES // STEP // 2, comps, 2 * SUBS, samples + 5 * LANES), jnp.bfloat16
            ),
            pltpu.VMEM((comps * tiles * LANES, spread), jnp.bfloat16),
            pltpu.VMEM((plane, SUBS, width), jnp.float32),
            pltpu.VMEM((deep, SUBS, width), jnp.float32),
            pltpu.VMEM((plane, SUBS, width), jnp.float32),
            pltpu.VMEM((deep, CORES, SUBS, width), jnp.float32),
            pltpu.VMEM((SUBS, width), jnp.float32),
            dma((plane,)),
            dma((deep * CORES,)),
            dma((deep * CORES,)),
            dma((plane,)),
            dma((plane,)),
            dma((deep * CORES,)),
            dma((plane,)),
            dma((deep * CORES,)),
            dma((1,)),
        ],
        compiler_params=pltpu.CompilerParams(collective_id=0, has_side_effects=True),
    )(templates)


def solution(mesh):
    placed = (P(("row", "col"), None, None),)
    return jax.shard_map(
        body, mesh=mesh, in_specs=placed, out_specs=P(("row", "col"), None), check_vma=False
    )
```

```python
import functools
import math

import jax
import jax.numpy as jnp
from jax import lax
from jax.experimental import pallas as pl
from jax.experimental.pallas import tpu as pltpu
from jax.sharding import PartitionSpec as P

LAGS = 512
LANES = 128
SUBS = 8
CORES = 2
STEP = 16
MESH = pl.DeviceIdType.MESH


def each(count, step):
    if count <= 16:
        for k in range(count):
            step(k)
    else:
        lax.fori_loop(0, count, lambda k, carry: (step(k), carry)[1], 0)


def when(condition, step):
    pl.when(condition)(step)


def kernel(
    rows,
    cols,
    x_hbm,
    out_ref,
    x_ref,
    stage,
    beside,
    column_blocks,
    lines_ref,
    flat,
    waves,
    shifts,
    answers,
    turned_rows,
    from_plane,
    from_column,
    total,
    block_sem,
    column_send_sem,
    column_sem,
    plane_sem,
    answer_sem,
    turned_sem,
    from_plane_sem,
    from_column_sem,
    table_sem,
    up_sem,
):
    n, comps, samples = x_ref.shape
    chunks = samples // LANES
    series = n * comps
    lines = series * chunks
    tall = rows // CORES
    wide = 2 ** int(math.log2(math.sqrt(cols)))
    deep = cols // wide
    plane = tall * wide
    width = total.shape[1]
    blocks = LAGS // STEP
    phases = LANES // STEP
    tiles = chunks + 1
    row = lax.axis_index("row")
    col = lax.axis_index("col")
    my_y, my_core = row // CORES, row % CORES
    my_z, my_x = col // wide, col % wide
    my_xy = my_y * wide + my_x
    other = 1 - my_core

    def place(xy, z, core):
        return (xy // wide) * CORES + core, z * wide + xy % wide

    def column(xy, z, core):
        return (((xy // wide) * CORES + core) * cols + z * wide + xy % wide) * n

    def mate(k):
        if plane & (plane - 1):
            return (my_xy + k) % plane
        found, bit = 0, 1
        while bit < plane:
            found, bit = found + (my_xy // bit + k // bit) % 2 * bit, bit * 2
        return found

    def mates(step):
        each(plane - 1, lambda k: step(mate(k + 1)))

    def compared(z, to):
        return (z > 0) & ((to == 0) | (to == z + 1) | ((to > 0) & (to < z - 1)))

    hosted = jnp.where(
        my_z == 0,
        deep - 1,
        jnp.where(my_z > 1, 1, 0) + jnp.maximum(deep - 2 - my_z, 0),
    )

    def above(step):
        for z in range(1, deep):
            for core in range(CORES):
                when(z > my_z, lambda: step(z, core))

    corner = plane - 1, deep - 1
    at_origin = (my_xy == 0) & (my_z == 0)
    at_corner = (my_xy == corner[0]) & (my_z == corner[1])
    at_foot = (my_xy == corner[0]) & (my_z == 0)

    barrier = pltpu.get_barrier_semaphore()

    def greet(xy, z, core):
        pl.semaphore_signal(barrier, inc=1, device_id=place(xy, z, core), device_id_type=MESH)

    def announce(z, core):
        pl.semaphore_signal(
            up_sem, inc=1, device_id=place(my_xy, z, core), device_id_type=MESH
        )

    taken = pltpu.make_async_copy(x_hbm, x_ref, table_sem.at[0])
    taken.start()
    mates(lambda xy: greet(xy, my_z, other))
    above(lambda z, core: greet(my_xy, z, core))
    greet(my_xy, my_z, other)
    for core in range(CORES):
        when(at_origin, lambda: greet(*corner, core))
    taken.wait()

    for t in range(n):
        x = x_ref[t]
        scale = lax.rsqrt(jnp.mean(x * x, axis=1, keepdims=True) + 1e-06) / math.sqrt(samples)
        rounded = (x * scale).astype(jnp.bfloat16).astype(jnp.float32)
        for q in range(chunks):
            stage[pl.ds(t * chunks + q, comps, stride=n * chunks), :] = rounded[
                :, q * LANES : (q + 1) * LANES
            ]
    column_blocks[my_z, my_core] = (
        stage[...].reshape(comps, n, chunks, LANES).astype(jnp.bfloat16)
    )
    pl.semaphore_wait(barrier, CORES * my_z + plane + jnp.where(at_corner, CORES, 0))

    mine = column_blocks.at[my_z, my_core]

    def to_column(z, core):
        return pltpu.make_async_remote_copy(
            src_ref=mine,
            dst_ref=mine,
            send_sem=column_send_sem.at[z * CORES + core],
            recv_sem=column_sem.at[my_z * CORES + my_core],
            device_id=place(my_xy, z, core),
            device_id_type=MESH,
        )

    def to_origin(core):
        return pltpu.make_async_remote_copy(
            src_ref=mine,
            dst_ref=column_blocks.at[deep, my_core],
            send_sem=column_send_sem.at[deep * CORES + core],
            recv_sem=column_sem.at[deep * CORES + my_core],
            device_id=place(0, 0, core),
            device_id_type=MESH,
        )

    def to_mate(xy):
        return pltpu.make_async_remote_copy(
            src_ref=mine,
            dst_ref=beside.at[my_xy],
            send_sem=block_sem.at[xy],
            recv_sem=plane_sem.at[my_xy],
            device_id=place(xy, my_z, other),
            device_id_type=MESH,
        )

    def from_above(z, core):
        block = column_blocks.at[z, core]
        return pltpu.make_async_remote_copy(
            src_ref=block,
            dst_ref=block,
            send_sem=column_send_sem.at[core],
            recv_sem=column_sem.at[z * CORES + core],
            device_id=place(my_xy, my_z, other),
            device_id_type=MESH,
        )

    def from_mate(xy):
        return pltpu.make_async_remote_copy(
            src_ref=mine,
            dst_ref=beside.at[xy],
            send_sem=block_sem.at[xy],
            recv_sem=plane_sem.at[xy],
            device_id=place(xy, my_z, other),
            device_id_type=MESH,
        )

    def send_to(z):
        to_column(z, my_core).start()
        to_column(z, other).start()

    when(my_z > 0, lambda: send_to(0))
    mates(lambda xy: to_mate(xy).start())
    to_column(my_z, other).start()
    def gone(z):
        for core in range(CORES):
            to_column(z, core).wait_send()


    for m in range(phases // 2):
        for c in range(comps):
            waves[m, c, :, :LANES] = jnp.zeros((2 * SUBS, LANES), jnp.bfloat16)
            waves[m, c, :, (chunks + 2) * LANES :] = jnp.zeros(
                (2 * SUBS, 3 * LANES), jnp.bfloat16
            )
    answers[...] = jnp.zeros(answers.shape, jnp.float32)

    def settle(k):
        if k == 0:
            block = stage[...]
        else:
            from_mate(mate(k)).wait_recv()
            block = beside[mate(k)].astype(jnp.float32).reshape(lines, LANES)
        lines_ref[k * lines : (k + 1) * lines, :] = block

    segments = LANES // STEP
    seats_of = segments // 2

    room = 2 * STEP

    def stand(g):
        held = range(2 * g, min(2 * g + 2, plane))
        for k in held:
            settle(k)
        local = jnp.concatenate(
            [
                lines_ref[pl.ds(2 * g * lines + q, len(held) * series, stride=chunks), :]
                for q in range(chunks)
            ]
            + [jnp.zeros((len(held) * series, LANES), jnp.float32)],
            axis=1,
        )
        for c in range(comps):
            parts = []
            for s in range(segments):
                k, t = s // seats_of, s % seats_of
                if k < len(held) and t < n:
                    r = k * series + c * n + t
                    line = jnp.broadcast_to(local[r : r + 1], (STEP, tiles * LANES))
                    line = pltpu.roll(line, 0, 1, stride=1, stride_axis=0)
                else:
                    line = jnp.zeros((STEP, tiles * LANES), jnp.float32)
                parts.append(line.astype(jnp.bfloat16))
            stood = jnp.concatenate(parts, axis=0).T
            at = slice(g * LANES, (g + 1) * LANES)
            shifts[c * samples : (c + 1) * samples, at] = stood[:samples]
            tail = comps * samples + c * room
            shifts[tail : tail + room, at] = stood[samples : samples + room]
        unused = comps * samples + comps * room
        shifts[unused:, g * LANES : (g + 1) * LANES] = jnp.zeros(
            (shifts.shape[0] - unused, LANES), jnp.bfloat16
        )

    for z in range(1, deep - 1):
        for core in range(CORES):
            when(my_z == z + 1, lambda: announce(z, core))
    when(my_z > 0, lambda: gone(0))
    for core in range(CORES):
        when(at_corner, lambda: to_origin(core).start())
    for z in range(1, deep - 2):
        when(my_z > z + 1, lambda: send_to(z))
    when((my_z > 0) & (my_z < deep - 1), lambda: pl.semaphore_wait(up_sem, CORES))
    for z in range(2, deep):
        when(my_z == z - 1, lambda: send_to(z))
    for g in range((plane + 1) // 2):
        stand(g)

    def answer(k):
        return pltpu.make_async_remote_copy(
            src_ref=answers.at[k],
            dst_ref=from_plane.at[my_xy],
            send_sem=answer_sem.at[k],
            recv_sem=from_plane_sem.at[my_xy],
            device_id=place(mate(k), my_z, other),
            device_id_type=MESH,
        )

    def give_back(z, core):
        return pltpu.make_async_remote_copy(
            src_ref=turned_rows.at[z],
            dst_ref=from_column.at[my_z, my_core],
            send_sem=turned_sem.at[z * CORES + core],
            recv_sem=from_column_sem.at[my_z * CORES + my_core],
            device_id=place(my_xy, z, core),
            device_id_type=MESH,
        )

    lane = lax.broadcasted_iota(jnp.int32, (SUBS, width), 1)
    tops = lax.broadcasted_iota(jnp.int32, (SUBS, width), 0)
    place_lane = lax.broadcasted_iota(jnp.int32, (SUBS, 2 * LANES), 1)
    seat = place_lane % STEP
    tail_lane = lax.broadcasted_iota(jnp.int32, (2 * SUBS, LANES), 1)

    def compare(z, kind, final=False):
        own, above_me = kind == "own", kind == "above"
        target = jnp.full((SUBS, width), -1, jnp.int32)
        for core in range(CORES):
            here = (tops >= core * n) & (tops < (core + 1) * n)
            seat_of = column(*corner, core) if kind == "corner" else column(my_xy, z, core)
            target = jnp.where(here, seat_of - core * n + tops, target)
        spot = lane == target

        def prepare(c):
            flat[c, : CORES * n * chunks] = (
                column_blocks[z, :, c].astype(jnp.float32).reshape(CORES * n * chunks, LANES)
            )
            wave = jnp.concatenate(
                [flat[c, pl.ds(q, SUBS, stride=chunks), :] for q in range(chunks)]
                + [jnp.zeros((SUBS, LANES), jnp.float32)],
                axis=1,
            )
            for m in range(phases // 2):
                pair = [
                    wave if b == 0 else pltpu.roll(wave, tiles * LANES - b * STEP, 1)
                    for b in (2 * m, 2 * m + 1)
                ]
                pair = jnp.concatenate(pair, axis=0).astype(jnp.bfloat16)
                waves[m, c, :, 2 * LANES : (chunks + 2) * LANES] = pair[:, :samples]
                waves[m, c, :, LANES : 2 * LANES] = pair[:, samples:]

        def lined_up(c, at, size):
            parts = []
            for p in range(0, blocks + 2, 2):
                start = at + p // phases * LANES
                parts.append(waves[p % phases // 2, c, :, start : start + size])
            return jnp.concatenate(parts, axis=0)

        def lined_up_tails():
            parts = []
            for p in range(0, blocks // 2, 2):
                joined = None
                for c in range(comps):
                    turn = p % phases // 2 - c
                    start = samples + (p // phases + turn // (phases // 2)) * LANES
                    piece = waves[turn % (phases // 2), c, :, start : start + LANES]
                    joined = piece if c == 0 else jnp.where(tail_lane < c * room, joined, piece)
                parts.append(joined)
            return jnp.concatenate(parts, axis=0)

        def products(g):
            at = slice(2 * g * LANES, 2 * (g + 1) * LANES)
            found = jnp.zeros(((blocks + 2) * SUBS, 2 * LANES), jnp.float32)
            for c in range(comps):
                for start in range(0, samples, 2 * LANES):
                    base = c * samples + start
                    found = found + jnp.dot(
                        lined_up(c, start, 2 * LANES),
                        shifts[base : base + 2 * LANES, at],
                        preferred_element_type=jnp.float32,
                    )
            middle = blocks // 2 * SUBS
            ends = jnp.dot(
                lined_up_tails(),
                shifts[comps * samples : comps * samples + LANES, at],
                preferred_element_type=jnp.float32,
            )
            return jnp.concatenate([found[:middle] + ends, found[middle:]], axis=0)

        wholes = shifts.shape[1] // (2 * LANES)
        parted = at_foot & (z == deep - 1)
        if above_me:
            for k in range(1, plane):
                when(parted & (mate(k) == 0), lambda: answer(k).start())
        if own:
            from_above(z, other).wait_recv()
        else:
            for core in range(CORES):
                from_above(z, core).wait_recv()
        for c in range(comps):
            prepare(c)

        turned = jnp.zeros((SUBS, width), jnp.float32)
        parts = []
        for g in range(wholes):
            found = products(g)

            def part(p):
                return found[p * SUBS : (p + 1) * SUBS]

            middle = part(1)
            for p in range(2, blocks):
                middle = jnp.maximum(middle, part(p))
            plain = jnp.maximum(middle, part(0))
            swapped = jnp.maximum(middle, jnp.where(seat == 0, part(blocks), part(0)))
            parts.append(swapped)
            for k, t, part_at, inside in seats(g):
                if own or (kind == "corner" and k):
                    break
                into = k if kind == "corner" else jnp.where(parted & (mate(k) == 0), plane, k)
                best = jnp.max(
                    jnp.where(inside, plain[:, part_at], -jnp.inf), axis=1, keepdims=True
                )
                answers[into, t : t + 1] += jnp.sum(
                    jnp.where(spot, best, 0.0), axis=0, keepdims=True
                )
        if kind == "corner":
            return
        if above_me:
            for k in range(1, plane):
                when(final & ~(parted & (mate(k) == 0)), lambda: answer(k).start())
        for g in range(wholes):
            for k, t, part_at, inside in seats(g):
                best = jnp.max(
                    jnp.where(inside, parts[g][:, part_at], -jnp.inf), axis=1, keepdims=True
                )
                core = other if k else my_core
                turned = jnp.where(lane == column(mate(k), my_z, core) + t, best, turned)
        turned_rows[z] = turned
        for core in range(CORES):
            if own:
                when(core != my_core, lambda: give_back(z, core).start())
            else:
                give_back(z, core).start()

    def seats(g):
        for s in range(2 * segments):
            k, t = g * 2 * segments // seats_of + s // seats_of, s % seats_of
            if k < plane and t < n:
                v = place_lane[:, :LANES] - s % segments * STEP
                part_at = slice(s // segments * LANES, (s // segments + 1) * LANES)
                yield k, t, part_at, (v >= 0) & (v < STEP)

    def one_by_one(i, carry):
        up = jnp.where(i == 0, my_z - 1, my_z + 1 + i)
        z = jnp.where(my_z == 0, i + 1, jnp.where(my_z > 1, up, my_z + 2 + i))
        compare(z, "above", i == hosted - 1)
        return carry

    lax.fori_loop(0, hosted, one_by_one, 0)
    compare(my_z, "own")
    when(at_origin, lambda: compare(deep, "corner"))

    total[...] = turned_rows[my_z]

    def collect(z, core):
        pltpu.make_async_remote_copy(
            src_ref=turned_rows.at[0],
            dst_ref=from_column.at[z, core],
            send_sem=turned_sem.at[z * CORES + core],
            recv_sem=from_column_sem.at[z * CORES + core],
            device_id=place(my_xy, my_z, other),
            device_id_type=MESH,
        ).wait_recv()
        total[...] += from_column[z, core]

    for z in range(deep):
        for core in range(CORES):
            when(
                compared(my_z, z) | ((z == my_z) & (core != my_core)),
                lambda: collect(z, core),
            )
    total[...] = pltpu.roll(total[...], (SUBS - my_core * n) % SUBS, 0)
    total[...] += answers[0]

    def hear(xy):
        pltpu.make_async_remote_copy(
            src_ref=answers.at[0],
            dst_ref=from_plane.at[xy],
            send_sem=answer_sem.at[0],
            recv_sem=from_plane_sem.at[xy],
            device_id=place(xy, my_z, other),
            device_id_type=MESH,
        ).wait_recv()
        total[...] += from_plane[xy]

    for z in range(1, deep):
        when(compared(my_z, z), lambda: gone(z))
    to_column(my_z, other).wait_send()
    mates(lambda xy: to_mate(xy).wait_send())
    when(hosted > 0, lambda: each(plane - 1, lambda k: answer(k + 1).wait_send()))
    for z in range(1, deep):
        for core in range(CORES):
            when(compared(z, my_z), lambda: give_back(z, core).wait_send())
    give_back(my_z, other).wait_send()
    for core in range(CORES):
        when(at_corner, lambda: to_origin(core).wait_send())
    when(hosted > 0, lambda: mates(hear))
    out_ref[...] = total[:n, : out_ref.shape[1]]


def body(templates):
    n, comps, samples = templates.shape
    rows = lax.axis_size("row")
    cols = lax.axis_size("col")
    chunks = samples // LANES
    series = n * comps
    lines = series * chunks
    wide = 2 ** int(math.log2(math.sqrt(cols)))
    deep = cols // wide
    plane = rows // CORES * wide
    out_width = rows * cols * n
    width = out_width + -out_width % LANES
    tiles = chunks + 1
    spread = plane * LANES // 2
    spread += -spread % (2 * LANES)
    dma = pltpu.SemaphoreType.DMA
    return pl.pallas_call(
        functools.partial(kernel, rows, cols),
        out_shape=pltpu.VMEM((n, out_width), jnp.float32),
        in_specs=[pl.BlockSpec(memory_space=pltpu.HBM)],
        out_specs=pl.BlockSpec(memory_space=pltpu.VMEM),
        scratch_shapes=[
            pltpu.VMEM(templates.shape, jnp.float32),
            pltpu.VMEM((lines, LANES), jnp.float32),
            pltpu.VMEM((plane, comps, n, chunks, LANES), jnp.bfloat16),
            pltpu.VMEM((deep + 1, CORES, comps, n, chunks, LANES), jnp.bfloat16),
            pltpu.VMEM((plane * lines, LANES), jnp.float32),
            pltpu.VMEM((comps, SUBS * chunks, LANES), jnp.float32),
            pltpu.VMEM(
                (LANES // STEP // 2, comps, 2 * SUBS, samples + 5 * LANES), jnp.bfloat16
            ),
            pltpu.VMEM((comps * samples + LANES, spread), jnp.bfloat16),
            pltpu.VMEM((plane + 1, SUBS, width), jnp.float32),
            pltpu.VMEM((deep, SUBS, width), jnp.float32),
            pltpu.VMEM((plane, SUBS, width), jnp.float32),
            pltpu.VMEM((deep, CORES, SUBS, width), jnp.float32),
            pltpu.VMEM((SUBS, width), jnp.float32),
            dma((plane,)),
            dma(((deep + 1) * CORES,)),
            dma(((deep + 1) * CORES,)),
            dma((plane,)),
            dma((plane,)),
            dma((deep * CORES,)),
            dma((plane,)),
            dma((deep * CORES,)),
            dma((1,)),
            pltpu.SemaphoreType.REGULAR,
        ],
        compiler_params=pltpu.CompilerParams(collective_id=0, has_side_effects=True),
    )(templates)


def solution(mesh):
    placed = (P(("row", "col"), None, None),)
    return jax.shard_map(
        body, mesh=mesh, in_specs=placed, out_specs=P(("row", "col"), None), check_vma=False
    )
```

```python
import functools
import math

import jax
import jax.numpy as jnp
from jax import lax
from jax.experimental import pallas as pl
from jax.experimental.pallas import tpu as pltpu
from jax.sharding import PartitionSpec as P

LAGS = 512
LANES = 128
SUBS = 8
CORES = 2
STEP = 16
MESH = pl.DeviceIdType.MESH


def each(count, step):
    if count <= 16:
        for k in range(count):
            step(k)
    else:
        lax.fori_loop(0, count, lambda k, carry: (step(k), carry)[1], 0)


def when(condition, step):
    pl.when(condition)(step)


def kernel(
    rows,
    cols,
    x_hbm,
    out_ref,
    x_ref,
    stage,
    beside,
    column_blocks,
    lines_ref,
    flat,
    waves,
    shifts,
    answers,
    turned_rows,
    from_plane,
    from_column,
    total,
    block_sem,
    column_send_sem,
    column_sem,
    plane_sem,
    answer_sem,
    turned_sem,
    from_plane_sem,
    from_column_sem,
    table_sem,
    up_sem,
):
    n, comps, samples = x_ref.shape
    chunks = samples // LANES
    series = n * comps
    lines = series * chunks
    tall = rows // CORES
    wide = 2 ** int(math.log2(math.sqrt(cols)))
    deep = cols // wide
    plane = tall * wide
    width = total.shape[1]
    blocks = LAGS // STEP
    phases = LANES // STEP
    tiles = chunks + 1
    row = lax.axis_index("row")
    col = lax.axis_index("col")
    my_y, my_core = row // CORES, row % CORES
    my_z, my_x = col // wide, col % wide
    my_xy = my_y * wide + my_x
    other = 1 - my_core

    def place(xy, z, core):
        return (xy // wide) * CORES + core, z * wide + xy % wide

    def column(xy, z, core):
        return (((xy // wide) * CORES + core) * cols + z * wide + xy % wide) * n

    def mate(k):
        if plane & (plane - 1):
            return (my_xy + k) % plane
        found, bit = 0, 1
        while bit < plane:
            found, bit = found + (my_xy // bit + k // bit) % 2 * bit, bit * 2
        return found

    def mates(step):
        each(plane - 1, lambda k: step(mate(k + 1)))

    def compared(z, to):
        return (z > 0) & ((to == 0) | (to == z + 1) | ((to > 0) & (to < z - 1)))

    hosted = jnp.where(
        my_z == 0,
        deep - 1,
        jnp.where(my_z > 1, 1, 0) + jnp.maximum(deep - 2 - my_z, 0),
    )

    def above(step):
        for z in range(1, deep):
            for core in range(CORES):
                when(z > my_z, lambda: step(z, core))

    corner = plane - 1, deep - 1
    at_origin = (my_xy == 0) & (my_z == 0)
    at_corner = (my_xy == corner[0]) & (my_z == corner[1])
    at_foot = (my_xy == corner[0]) & (my_z == 0)

    barrier = pltpu.get_barrier_semaphore()

    def greet(xy, z, core):
        pl.semaphore_signal(barrier, inc=1, device_id=place(xy, z, core), device_id_type=MESH)

    def announce(z, core):
        pl.semaphore_signal(
            up_sem, inc=1, device_id=place(my_xy, z, core), device_id_type=MESH
        )

    taken = pltpu.make_async_copy(x_hbm, x_ref, table_sem.at[0])
    taken.start()
    mates(lambda xy: greet(xy, my_z, other))
    above(lambda z, core: greet(my_xy, z, core))
    greet(my_xy, my_z, other)
    for core in range(CORES):
        when(at_origin, lambda: greet(*corner, core))
    taken.wait()

    for t in range(n):
        x = x_ref[t]
        scale = lax.rsqrt(jnp.mean(x * x, axis=1, keepdims=True) + 1e-06) / math.sqrt(samples)
        rounded = (x * scale).astype(jnp.bfloat16).astype(jnp.float32)
        for q in range(chunks):
            stage[pl.ds(t * chunks + q, comps, stride=n * chunks), :] = rounded[
                :, q * LANES : (q + 1) * LANES
            ]
    column_blocks[my_z, my_core] = (
        stage[...].reshape(comps, n, chunks, LANES).astype(jnp.bfloat16)
    )
    pl.semaphore_wait(barrier, CORES * my_z + plane + jnp.where(at_corner, CORES, 0))

    mine = column_blocks.at[my_z, my_core]

    def to_column(z, core):
        return pltpu.make_async_remote_copy(
            src_ref=mine,
            dst_ref=mine,
            send_sem=column_send_sem.at[z * CORES + core],
            recv_sem=column_sem.at[my_z * CORES + my_core],
            device_id=place(my_xy, z, core),
            device_id_type=MESH,
        )

    def to_origin(core):
        return pltpu.make_async_remote_copy(
            src_ref=mine,
            dst_ref=column_blocks.at[deep, my_core],
            send_sem=column_send_sem.at[deep * CORES + core],
            recv_sem=column_sem.at[deep * CORES + my_core],
            device_id=place(0, 0, core),
            device_id_type=MESH,
        )

    def to_mate(xy):
        return pltpu.make_async_remote_copy(
            src_ref=mine,
            dst_ref=beside.at[my_xy],
            send_sem=block_sem.at[xy],
            recv_sem=plane_sem.at[my_xy],
            device_id=place(xy, my_z, other),
            device_id_type=MESH,
        )

    def from_above(z, core):
        block = column_blocks.at[z, core]
        return pltpu.make_async_remote_copy(
            src_ref=block,
            dst_ref=block,
            send_sem=column_send_sem.at[core],
            recv_sem=column_sem.at[z * CORES + core],
            device_id=place(my_xy, my_z, other),
            device_id_type=MESH,
        )

    def hand_over():
        block = column_blocks.at[deep - 1, other]
        return pltpu.make_async_remote_copy(
            src_ref=block,
            dst_ref=block,
            send_sem=column_send_sem.at[(deep - 1) * CORES],
            recv_sem=column_sem.at[(deep - 1) * CORES + other],
            device_id=place(my_xy, my_z, other),
            device_id_type=MESH,
        )

    def from_mate(xy):
        return pltpu.make_async_remote_copy(
            src_ref=mine,
            dst_ref=beside.at[xy],
            send_sem=block_sem.at[xy],
            recv_sem=plane_sem.at[xy],
            device_id=place(xy, my_z, other),
            device_id_type=MESH,
        )

    def send_to(z):
        if z == 0:
            when(~at_corner, lambda: to_column(z, my_core).start())
        else:
            to_column(z, my_core).start()
        to_column(z, other).start()

    when(my_z > 0, lambda: send_to(0))
    mates(lambda xy: to_mate(xy).start())
    to_column(my_z, other).start()
    def gone(z):
        if z == 0:
            when(~at_corner, lambda: to_column(z, my_core).wait_send())
        else:
            to_column(z, my_core).wait_send()
        to_column(z, other).wait_send()


    for m in range(phases // 2):
        for c in range(comps):
            waves[m, c, :, :LANES] = jnp.zeros((2 * SUBS, LANES), jnp.bfloat16)
            waves[m, c, :, (chunks + 2) * LANES :] = jnp.zeros(
                (2 * SUBS, 3 * LANES), jnp.bfloat16
            )
    answers[...] = jnp.zeros(answers.shape, jnp.float32)

    def settle(k):
        if k == 0:
            block = stage[...]
        else:
            from_mate(mate(k)).wait_recv()
            block = beside[mate(k)].astype(jnp.float32).reshape(lines, LANES)
        lines_ref[k * lines : (k + 1) * lines, :] = block

    segments = LANES // STEP
    seats_of = segments // 2

    room = 2 * STEP

    def stand(g):
        held = range(2 * g, min(2 * g + 2, plane))
        for k in held:
            settle(k)
        local = jnp.concatenate(
            [
                lines_ref[pl.ds(2 * g * lines + q, len(held) * series, stride=chunks), :]
                for q in range(chunks)
            ]
            + [jnp.zeros((len(held) * series, LANES), jnp.float32)],
            axis=1,
        )
        for c in range(comps):
            parts = []
            for s in range(segments):
                k, t = s // seats_of, s % seats_of
                if k < len(held) and t < n:
                    r = k * series + c * n + t
                    line = jnp.broadcast_to(local[r : r + 1], (STEP, tiles * LANES))
                    line = pltpu.roll(line, 0, 1, stride=1, stride_axis=0)
                else:
                    line = jnp.zeros((STEP, tiles * LANES), jnp.float32)
                parts.append(line.astype(jnp.bfloat16))
            stood = jnp.concatenate(parts, axis=0).T
            at = slice(g * LANES, (g + 1) * LANES)
            shifts[c * samples : (c + 1) * samples, at] = stood[:samples]
            tail = comps * samples + c * room
            shifts[tail : tail + room, at] = stood[samples : samples + room]
        unused = comps * samples + comps * room
        shifts[unused:, g * LANES : (g + 1) * LANES] = jnp.zeros(
            (shifts.shape[0] - unused, LANES), jnp.bfloat16
        )

    for z in range(1, deep - 1):
        for core in range(CORES):
            when(my_z == z + 1, lambda: announce(z, core))
    when(my_z > 0, lambda: gone(0))
    for core in range(CORES):
        when(at_corner, lambda: to_origin(core).start())
    for z in range(1, deep - 2):
        when(my_z > z + 1, lambda: send_to(z))
    when((my_z > 0) & (my_z < deep - 1), lambda: pl.semaphore_wait(up_sem, CORES))
    for z in range(2, deep):
        when(my_z == z - 1, lambda: send_to(z))
    for g in range((plane + 1) // 2):
        stand(g)

    def answer(k):
        return pltpu.make_async_remote_copy(
            src_ref=answers.at[k],
            dst_ref=from_plane.at[my_xy],
            send_sem=answer_sem.at[k],
            recv_sem=from_plane_sem.at[my_xy],
            device_id=place(mate(k), my_z, other),
            device_id_type=MESH,
        )

    def give_back(z, core):
        return pltpu.make_async_remote_copy(
            src_ref=turned_rows.at[z],
            dst_ref=from_column.at[my_z, my_core],
            send_sem=turned_sem.at[z * CORES + core],
            recv_sem=from_column_sem.at[my_z * CORES + my_core],
            device_id=place(my_xy, z, core),
            device_id_type=MESH,
        )

    lane = lax.broadcasted_iota(jnp.int32, (SUBS, width), 1)
    tops = lax.broadcasted_iota(jnp.int32, (SUBS, width), 0)
    place_lane = lax.broadcasted_iota(jnp.int32, (SUBS, 2 * LANES), 1)
    seat = place_lane % STEP
    tail_lane = lax.broadcasted_iota(jnp.int32, (2 * SUBS, LANES), 1)

    def compare(z, kind, final=False):
        own, above_me = kind == "own", kind == "above"
        target = jnp.full((SUBS, width), -1, jnp.int32)
        for core in range(CORES):
            here = (tops >= core * n) & (tops < (core + 1) * n)
            seat_of = column(*corner, core) if kind == "corner" else column(my_xy, z, core)
            target = jnp.where(here, seat_of - core * n + tops, target)
        spot = lane == target

        def prepare(c):
            flat[c, : CORES * n * chunks] = (
                column_blocks[z, :, c].astype(jnp.float32).reshape(CORES * n * chunks, LANES)
            )
            wave = jnp.concatenate(
                [flat[c, pl.ds(q, SUBS, stride=chunks), :] for q in range(chunks)]
                + [jnp.zeros((SUBS, LANES), jnp.float32)],
                axis=1,
            )
            for m in range(phases // 2):
                pair = [
                    wave if b == 0 else pltpu.roll(wave, tiles * LANES - b * STEP, 1)
                    for b in (2 * m, 2 * m + 1)
                ]
                pair = jnp.concatenate(pair, axis=0).astype(jnp.bfloat16)
                waves[m, c, :, 2 * LANES : (chunks + 2) * LANES] = pair[:, :samples]
                waves[m, c, :, LANES : 2 * LANES] = pair[:, samples:]

        def lined_up(c, at, size):
            parts = []
            for p in range(0, blocks + 2, 2):
                start = at + p // phases * LANES
                parts.append(waves[p % phases // 2, c, :, start : start + size])
            return jnp.concatenate(parts, axis=0)

        def lined_up_tails():
            parts = []
            for p in range(0, blocks // 2, 2):
                joined = None
                for c in range(comps):
                    turn = p % phases // 2 - c
                    start = samples + (p // phases + turn // (phases // 2)) * LANES
                    piece = waves[turn % (phases // 2), c, :, start : start + LANES]
                    joined = piece if c == 0 else jnp.where(tail_lane < c * room, joined, piece)
                parts.append(joined)
            return jnp.concatenate(parts, axis=0)

        def products(g):
            at = slice(2 * g * LANES, 2 * (g + 1) * LANES)
            found = jnp.zeros(((blocks + 2) * SUBS, 2 * LANES), jnp.float32)
            for c in range(comps):
                for start in range(0, samples, 2 * LANES):
                    base = c * samples + start
                    found = found + jnp.dot(
                        lined_up(c, start, 2 * LANES),
                        shifts[base : base + 2 * LANES, at],
                        preferred_element_type=jnp.float32,
                    )
            middle = blocks // 2 * SUBS
            ends = jnp.dot(
                lined_up_tails(),
                shifts[comps * samples : comps * samples + LANES, at],
                preferred_element_type=jnp.float32,
            )
            return jnp.concatenate([found[:middle] + ends, found[middle:]], axis=0)

        wholes = shifts.shape[1] // (2 * LANES)
        parted = at_foot & (z == deep - 1)
        if above_me:
            for k in range(1, plane):
                when(parted & (mate(k) == 0), lambda: answer(k).start())
        if own:
            from_above(z, other).wait_recv()
        else:
            from_above(z, other).wait_recv()
            if above_me:
                when(parted, lambda: hand_over().start())
            from_above(z, my_core).wait_recv()
        for c in range(comps):
            prepare(c)

        turned = jnp.zeros((SUBS, width), jnp.float32)
        parts = []
        for g in range(wholes):
            found = products(g)

            def part(p):
                return found[p * SUBS : (p + 1) * SUBS]

            middle = part(1)
            for p in range(2, blocks):
                middle = jnp.maximum(middle, part(p))
            plain = jnp.maximum(middle, part(0))
            swapped = jnp.maximum(middle, jnp.where(seat == 0, part(blocks), part(0)))
            parts.append(swapped)
            for k, t, part_at, inside in seats(g):
                if own or (kind == "corner" and k):
                    break
                into = k if kind == "corner" else jnp.where(parted & (mate(k) == 0), plane, k)
                best = jnp.max(
                    jnp.where(inside, plain[:, part_at], -jnp.inf), axis=1, keepdims=True
                )
                answers[into, t : t + 1] += jnp.sum(
                    jnp.where(spot, best, 0.0), axis=0, keepdims=True
                )
        if kind == "corner":
            return
        if above_me:
            for k in range(1, plane):
                when(final & ~(parted & (mate(k) == 0)), lambda: answer(k).start())
        for g in range(wholes):
            for k, t, part_at, inside in seats(g):
                best = jnp.max(
                    jnp.where(inside, parts[g][:, part_at], -jnp.inf), axis=1, keepdims=True
                )
                core = other if k else my_core
                turned = jnp.where(lane == column(mate(k), my_z, core) + t, best, turned)
        turned_rows[z] = turned
        for core in range(CORES):
            if own:
                when(core != my_core, lambda: give_back(z, core).start())
            else:
                give_back(z, core).start()

    def seats(g):
        for s in range(2 * segments):
            k, t = g * 2 * segments // seats_of + s // seats_of, s % seats_of
            if k < plane and t < n:
                v = place_lane[:, :LANES] - s % segments * STEP
                part_at = slice(s // segments * LANES, (s // segments + 1) * LANES)
                yield k, t, part_at, (v >= 0) & (v < STEP)

    def one_by_one(i, carry):
        up = jnp.where(i == 0, my_z - 1, my_z + 1 + i)
        z = jnp.where(my_z == 0, i + 1, jnp.where(my_z > 1, up, my_z + 2 + i))
        compare(z, "above", i == hosted - 1)
        return carry

    late_own = (my_z == 0) & (my_xy > 0)
    when(~late_own, lambda: compare(my_z, "own"))
    lax.fori_loop(0, hosted, one_by_one, 0)
    when(late_own, lambda: compare(my_z, "own"))
    when(at_origin, lambda: compare(deep, "corner"))

    total[...] = turned_rows[my_z]

    def collect(z, core):
        pltpu.make_async_remote_copy(
            src_ref=turned_rows.at[0],
            dst_ref=from_column.at[z, core],
            send_sem=turned_sem.at[z * CORES + core],
            recv_sem=from_column_sem.at[z * CORES + core],
            device_id=place(my_xy, my_z, other),
            device_id_type=MESH,
        ).wait_recv()
        total[...] += from_column[z, core]

    for z in range(deep):
        for core in range(CORES):
            when(
                compared(my_z, z) | ((z == my_z) & (core != my_core)),
                lambda: collect(z, core),
            )
    total[...] = pltpu.roll(total[...], (SUBS - my_core * n) % SUBS, 0)
    total[...] += answers[0]

    def hear(xy):
        pltpu.make_async_remote_copy(
            src_ref=answers.at[0],
            dst_ref=from_plane.at[xy],
            send_sem=answer_sem.at[0],
            recv_sem=from_plane_sem.at[xy],
            device_id=place(xy, my_z, other),
            device_id_type=MESH,
        ).wait_recv()
        total[...] += from_plane[xy]

    for z in range(1, deep):
        when(compared(my_z, z), lambda: gone(z))
    to_column(my_z, other).wait_send()
    mates(lambda xy: to_mate(xy).wait_send())
    when(hosted > 0, lambda: each(plane - 1, lambda k: answer(k + 1).wait_send()))
    for z in range(1, deep):
        for core in range(CORES):
            when(compared(z, my_z), lambda: give_back(z, core).wait_send())
    give_back(my_z, other).wait_send()
    for core in range(CORES):
        when(at_corner, lambda: to_origin(core).wait_send())
    when(at_foot, lambda: hand_over().wait_send())
    when(hosted > 0, lambda: mates(hear))
    out_ref[...] = total[:n, : out_ref.shape[1]]


def body(templates):
    n, comps, samples = templates.shape
    rows = lax.axis_size("row")
    cols = lax.axis_size("col")
    chunks = samples // LANES
    series = n * comps
    lines = series * chunks
    wide = 2 ** int(math.log2(math.sqrt(cols)))
    deep = cols // wide
    plane = rows // CORES * wide
    out_width = rows * cols * n
    width = out_width + -out_width % LANES
    tiles = chunks + 1
    spread = plane * LANES // 2
    spread += -spread % (2 * LANES)
    dma = pltpu.SemaphoreType.DMA
    return pl.pallas_call(
        functools.partial(kernel, rows, cols),
        out_shape=pltpu.VMEM((n, out_width), jnp.float32),
        in_specs=[pl.BlockSpec(memory_space=pltpu.HBM)],
        out_specs=pl.BlockSpec(memory_space=pltpu.VMEM),
        scratch_shapes=[
            pltpu.VMEM(templates.shape, jnp.float32),
            pltpu.VMEM((lines, LANES), jnp.float32),
            pltpu.VMEM((plane, comps, n, chunks, LANES), jnp.bfloat16),
            pltpu.VMEM((deep + 1, CORES, comps, n, chunks, LANES), jnp.bfloat16),
            pltpu.VMEM((plane * lines, LANES), jnp.float32),
            pltpu.VMEM((comps, SUBS * chunks, LANES), jnp.float32),
            pltpu.VMEM(
                (LANES // STEP // 2, comps, 2 * SUBS, samples + 5 * LANES), jnp.bfloat16
            ),
            pltpu.VMEM((comps * samples + LANES, spread), jnp.bfloat16),
            pltpu.VMEM((plane + 1, SUBS, width), jnp.float32),
            pltpu.VMEM((deep, SUBS, width), jnp.float32),
            pltpu.VMEM((plane, SUBS, width), jnp.float32),
            pltpu.VMEM((deep, CORES, SUBS, width), jnp.float32),
            pltpu.VMEM((SUBS, width), jnp.float32),
            dma((plane,)),
            dma(((deep + 1) * CORES,)),
            dma(((deep + 1) * CORES,)),
            dma((plane,)),
            dma((plane,)),
            dma((deep * CORES,)),
            dma((plane,)),
            dma((deep * CORES,)),
            dma((1,)),
            pltpu.SemaphoreType.REGULAR,
        ],
        compiler_params=pltpu.CompilerParams(collective_id=0, has_side_effects=True),
    )(templates)


def solution(mesh):
    placed = (P(("row", "col"), None, None),)
    return jax.shard_map(
        body, mesh=mesh, in_specs=placed, out_specs=P(("row", "col"), None), check_vma=False
    )
```

```python
import functools
import math

import jax
import jax.numpy as jnp
from jax import lax
from jax.experimental import pallas as pl
from jax.experimental.pallas import tpu as pltpu
from jax.sharding import PartitionSpec as P

LAGS = 512
LANES = 128
SUBS = 8
CORES = 2
STEP = 16
MESH = pl.DeviceIdType.MESH


def each(count, step):
    if count <= 16:
        for k in range(count):
            step(k)
    else:
        lax.fori_loop(0, count, lambda k, carry: (step(k), carry)[1], 0)


def when(condition, step):
    pl.when(condition)(step)


def kernel(
    rows,
    cols,
    x_hbm,
    out_ref,
    x_ref,
    stage,
    beside,
    column_blocks,
    lines_ref,
    flat,
    waves,
    shifts,
    answers,
    turned_rows,
    from_plane,
    from_column,
    total,
    block_sem,
    column_send_sem,
    column_sem,
    plane_sem,
    answer_sem,
    turned_sem,
    from_plane_sem,
    from_column_sem,
    table_sem,
    up_sem,
    mate_sem,
):
    n, comps, samples = x_ref.shape
    chunks = samples // LANES
    series = n * comps
    lines = series * chunks
    tall = rows // CORES
    wide = 2 ** int(math.log2(math.sqrt(cols)))
    deep = cols // wide
    plane = tall * wide
    width = total.shape[1]
    blocks = LAGS // STEP
    phases = LANES // STEP
    tiles = chunks + 1
    row = lax.axis_index("row")
    col = lax.axis_index("col")
    my_y, my_core = row // CORES, row % CORES
    my_z, my_x = col // wide, col % wide
    my_xy = my_y * wide + my_x
    other = 1 - my_core

    def place(xy, z, core):
        return (xy // wide) * CORES + core, z * wide + xy % wide

    def column(xy, z, core):
        return (((xy // wide) * CORES + core) * cols + z * wide + xy % wide) * n

    def mate(k):
        if plane & (plane - 1):
            return (my_xy + k) % plane
        found, bit = 0, 1
        while bit < plane:
            found, bit = found + (my_xy // bit + k // bit) % 2 * bit, bit * 2
        return found

    def mates(step):
        each(plane - 1, lambda k: step(mate(k + 1)))

    def compared(z, to):
        return (z > 0) & ((to == 0) | (to == z + 1) | ((to > 0) & (to < z - 1)))

    hosted = jnp.where(
        my_z == 0,
        deep - 1,
        jnp.where(my_z > 1, 1, 0) + jnp.maximum(deep - 2 - my_z, 0),
    )

    def above(step):
        for z in range(1, deep):
            for core in range(CORES):
                when(z > my_z, lambda: step(z, core))

    corner = plane - 1, deep - 1
    at_origin = (my_xy == 0) & (my_z == 0)
    at_corner = (my_xy == corner[0]) & (my_z == corner[1])
    at_foot = (my_xy == corner[0]) & (my_z == 0)

    barrier = pltpu.get_barrier_semaphore()

    def greet(xy, z, core):
        pl.semaphore_signal(barrier, inc=1, device_id=place(xy, z, core), device_id_type=MESH)

    def announce(z, core):
        pl.semaphore_signal(
            up_sem, inc=1, device_id=place(my_xy, z, core), device_id_type=MESH
        )

    taken = pltpu.make_async_copy(x_hbm, x_ref, table_sem.at[0])
    taken.start()
    hub = plane - 1
    at_hub = my_xy == hub
    for core in range(CORES):
        when((my_z > 0) & ~at_hub, lambda: greet(hub, my_z, core))
    when(my_z == 0, lambda: mates(lambda xy: greet(xy, my_z, other)))
    above(lambda z, core: greet(my_xy, z, core))
    greet(my_xy, my_z, other)
    for core in range(CORES):
        when(at_origin, lambda: greet(*corner, core))
    waited = CORES * my_z + 1 + jnp.where(at_hub, CORES * (plane - 1), 0)
    waited = waited + jnp.where(at_corner, CORES, 0)
    when(my_z > 0, lambda: pl.semaphore_wait(barrier, waited))

    def admit(xy):
        pl.semaphore_signal(
            mate_sem, inc=1, device_id=place(xy, my_z, other), device_id_type=MESH
        )

    when((my_z > 0) & at_hub, lambda: mates(admit))
    for z in range(1, deep - 1):
        for core in range(CORES):
            when(my_z == z + 1, lambda: announce(z, core))
    taken.wait()

    for t in range(n):
        x = x_ref[t]
        scale = lax.rsqrt(jnp.mean(x * x, axis=1, keepdims=True) + 1e-06) / math.sqrt(samples)
        rounded = (x * scale).astype(jnp.bfloat16).astype(jnp.float32)
        for q in range(chunks):
            stage[pl.ds(t * chunks + q, comps, stride=n * chunks), :] = rounded[
                :, q * LANES : (q + 1) * LANES
            ]
    column_blocks[my_z, my_core] = (
        stage[...].reshape(comps, n, chunks, LANES).astype(jnp.bfloat16)
    )

    when(my_z == 0, lambda: pl.semaphore_wait(barrier, plane))

    mine = column_blocks.at[my_z, my_core]

    def to_column(z, core):
        return pltpu.make_async_remote_copy(
            src_ref=mine,
            dst_ref=mine,
            send_sem=column_send_sem.at[z * CORES + core],
            recv_sem=column_sem.at[my_z * CORES + my_core],
            device_id=place(my_xy, z, core),
            device_id_type=MESH,
        )

    def to_origin(core):
        return pltpu.make_async_remote_copy(
            src_ref=mine,
            dst_ref=column_blocks.at[deep, my_core],
            send_sem=column_send_sem.at[deep * CORES + core],
            recv_sem=column_sem.at[deep * CORES + my_core],
            device_id=place(0, 0, core),
            device_id_type=MESH,
        )

    def to_mate(xy):
        return pltpu.make_async_remote_copy(
            src_ref=mine,
            dst_ref=beside.at[my_xy],
            send_sem=block_sem.at[xy],
            recv_sem=plane_sem.at[my_xy],
            device_id=place(xy, my_z, other),
            device_id_type=MESH,
        )

    def from_above(z, core):
        block = column_blocks.at[z, core]
        return pltpu.make_async_remote_copy(
            src_ref=block,
            dst_ref=block,
            send_sem=column_send_sem.at[core],
            recv_sem=column_sem.at[z * CORES + core],
            device_id=place(my_xy, my_z, other),
            device_id_type=MESH,
        )

    def hand_over():
        block = column_blocks.at[deep - 1, other]
        return pltpu.make_async_remote_copy(
            src_ref=block,
            dst_ref=block,
            send_sem=column_send_sem.at[(deep - 1) * CORES],
            recv_sem=column_sem.at[(deep - 1) * CORES + other],
            device_id=place(my_xy, my_z, other),
            device_id_type=MESH,
        )

    def from_mate(xy):
        return pltpu.make_async_remote_copy(
            src_ref=mine,
            dst_ref=beside.at[xy],
            send_sem=block_sem.at[xy],
            recv_sem=plane_sem.at[xy],
            device_id=place(xy, my_z, other),
            device_id_type=MESH,
        )

    def send_to(z):
        if z == 0:
            when(~at_corner, lambda: to_column(z, my_core).start())
        else:
            to_column(z, my_core).start()
        to_column(z, other).start()

    when(my_z > 0, lambda: send_to(0))
    for core in range(CORES):
        when(at_corner, lambda: to_origin(core).start())
    to_column(my_z, other).start()
    when((my_z > 0) & ~at_hub, lambda: pl.semaphore_wait(mate_sem, 1))
    mates(lambda xy: to_mate(xy).start())
    def gone(z):
        if z == 0:
            when(~at_corner, lambda: to_column(z, my_core).wait_send())
        else:
            to_column(z, my_core).wait_send()
        to_column(z, other).wait_send()


    for m in range(phases // 2):
        for c in range(comps):
            waves[m, c, :, :LANES] = jnp.zeros((2 * SUBS, LANES), jnp.bfloat16)
            waves[m, c, :, (chunks + 2) * LANES :] = jnp.zeros(
                (2 * SUBS, 3 * LANES), jnp.bfloat16
            )
    answers[...] = jnp.zeros(answers.shape, jnp.float32)

    def settle(k):
        if k == 0:
            block = stage[...]
        else:
            from_mate(mate(k)).wait_recv()
            block = beside[mate(k)].astype(jnp.float32).reshape(lines, LANES)
        lines_ref[k * lines : (k + 1) * lines, :] = block

    segments = LANES // STEP
    seats_of = segments // 2

    room = 2 * STEP

    def stand(g):
        held = range(2 * g, min(2 * g + 2, plane))
        for k in held:
            settle(k)
        local = jnp.concatenate(
            [
                lines_ref[pl.ds(2 * g * lines + q, len(held) * series, stride=chunks), :]
                for q in range(chunks)
            ]
            + [jnp.zeros((len(held) * series, LANES), jnp.float32)],
            axis=1,
        )
        for c in range(comps):
            parts = []
            for s in range(segments):
                k, t = s // seats_of, s % seats_of
                if k < len(held) and t < n:
                    r = k * series + c * n + t
                    line = jnp.broadcast_to(local[r : r + 1], (STEP, tiles * LANES))
                    line = pltpu.roll(line, 0, 1, stride=1, stride_axis=0)
                else:
                    line = jnp.zeros((STEP, tiles * LANES), jnp.float32)
                parts.append(line.astype(jnp.bfloat16))
            stood = jnp.concatenate(parts, axis=0).T
            at = slice(g * LANES, (g + 1) * LANES)
            shifts[c * samples : (c + 1) * samples, at] = stood[:samples]
            tail = comps * samples + c * room
            shifts[tail : tail + room, at] = stood[samples : samples + room]
        unused = comps * samples + comps * room
        shifts[unused:, g * LANES : (g + 1) * LANES] = jnp.zeros(
            (shifts.shape[0] - unused, LANES), jnp.bfloat16
        )

    when(my_z > 0, lambda: gone(0))
    for z in range(1, deep - 2):
        when(my_z > z + 1, lambda: send_to(z))
    when((my_z > 0) & (my_z < deep - 1), lambda: pl.semaphore_wait(up_sem, CORES))
    for z in range(2, deep):
        when(my_z == z - 1, lambda: send_to(z))
    for g in range((plane + 1) // 2):
        stand(g)

    def answer(k):
        return pltpu.make_async_remote_copy(
            src_ref=answers.at[k],
            dst_ref=from_plane.at[my_xy],
            send_sem=answer_sem.at[k],
            recv_sem=from_plane_sem.at[my_xy],
            device_id=place(mate(k), my_z, other),
            device_id_type=MESH,
        )

    def give_back(z, core):
        return pltpu.make_async_remote_copy(
            src_ref=turned_rows.at[z],
            dst_ref=from_column.at[my_z, my_core],
            send_sem=turned_sem.at[z * CORES + core],
            recv_sem=from_column_sem.at[my_z * CORES + my_core],
            device_id=place(my_xy, z, core),
            device_id_type=MESH,
        )

    lane = lax.broadcasted_iota(jnp.int32, (SUBS, width), 1)
    tops = lax.broadcasted_iota(jnp.int32, (SUBS, width), 0)
    place_lane = lax.broadcasted_iota(jnp.int32, (SUBS, 2 * LANES), 1)
    seat = place_lane % STEP
    tail_lane = lax.broadcasted_iota(jnp.int32, (2 * SUBS, LANES), 1)

    def compare(z, kind, final=False):
        own, above_me = kind == "own", kind == "above"
        target = jnp.full((SUBS, width), -1, jnp.int32)
        for core in range(CORES):
            here = (tops >= core * n) & (tops < (core + 1) * n)
            seat_of = column(*corner, core) if kind == "corner" else column(my_xy, z, core)
            target = jnp.where(here, seat_of - core * n + tops, target)
        spot = lane == target

        def prepare(c):
            flat[c, : CORES * n * chunks] = (
                column_blocks[z, :, c].astype(jnp.float32).reshape(CORES * n * chunks, LANES)
            )
            wave = jnp.concatenate(
                [flat[c, pl.ds(q, SUBS, stride=chunks), :] for q in range(chunks)]
                + [jnp.zeros((SUBS, LANES), jnp.float32)],
                axis=1,
            )
            for m in range(phases // 2):
                pair = [
                    wave if b == 0 else pltpu.roll(wave, tiles * LANES - b * STEP, 1)
                    for b in (2 * m, 2 * m + 1)
                ]
                pair = jnp.concatenate(pair, axis=0).astype(jnp.bfloat16)
                waves[m, c, :, 2 * LANES : (chunks + 2) * LANES] = pair[:, :samples]
                waves[m, c, :, LANES : 2 * LANES] = pair[:, samples:]

        def lined_up(c, at, size):
            parts = []
            for p in range(0, blocks + 2, 2):
                start = at + p // phases * LANES
                parts.append(waves[p % phases // 2, c, :, start : start + size])
            return jnp.concatenate(parts, axis=0)

        def lined_up_tails():
            parts = []
            for p in range(0, blocks // 2, 2):
                joined = None
                for c in range(comps):
                    turn = p % phases // 2 - c
                    start = samples + (p // phases + turn // (phases // 2)) * LANES
                    piece = waves[turn % (phases // 2), c, :, start : start + LANES]
                    joined = piece if c == 0 else jnp.where(tail_lane < c * room, joined, piece)
                parts.append(joined)
            return jnp.concatenate(parts, axis=0)

        def products(g):
            at = slice(2 * g * LANES, 2 * (g + 1) * LANES)
            found = jnp.zeros(((blocks + 2) * SUBS, 2 * LANES), jnp.float32)
            for c in range(comps):
                for start in range(0, samples, 2 * LANES):
                    base = c * samples + start
                    found = found + jnp.dot(
                        lined_up(c, start, 2 * LANES),
                        shifts[base : base + 2 * LANES, at],
                        preferred_element_type=jnp.float32,
                    )
            middle = blocks // 2 * SUBS
            ends = jnp.dot(
                lined_up_tails(),
                shifts[comps * samples : comps * samples + LANES, at],
                preferred_element_type=jnp.float32,
            )
            return jnp.concatenate([found[:middle] + ends, found[middle:]], axis=0)

        wholes = shifts.shape[1] // (2 * LANES)
        parted = at_foot & (z == deep - 1)
        if above_me:
            for k in range(1, plane):
                when(parted & (mate(k) == 0), lambda: answer(k).start())
        if own:
            from_above(z, other).wait_recv()
        else:
            from_above(z, other).wait_recv()
            if above_me:
                when(parted, lambda: hand_over().start())
            from_above(z, my_core).wait_recv()
        for c in range(comps):
            prepare(c)

        turned = jnp.zeros((SUBS, width), jnp.float32)
        parts = []
        for g in range(wholes):
            found = products(g)

            def part(p):
                return found[p * SUBS : (p + 1) * SUBS]

            middle = part(1)
            for p in range(2, blocks):
                middle = jnp.maximum(middle, part(p))
            plain = jnp.maximum(middle, part(0))
            swapped = jnp.maximum(middle, jnp.where(seat == 0, part(blocks), part(0)))
            parts.append(swapped)
            for k, t, part_at, inside in seats(g):
                if own or (kind == "corner" and k):
                    break
                into = k if kind == "corner" else jnp.where(parted & (mate(k) == 0), plane, k)
                best = jnp.max(
                    jnp.where(inside, plain[:, part_at], -jnp.inf), axis=1, keepdims=True
                )
                answers[into, t : t + 1] += jnp.sum(
                    jnp.where(spot, best, 0.0), axis=0, keepdims=True
                )
        if kind == "corner":
            return
        if above_me:
            for k in range(1, plane):
                when(final & ~(parted & (mate(k) == 0)), lambda: answer(k).start())
        for g in range(wholes):
            for k, t, part_at, inside in seats(g):
                best = jnp.max(
                    jnp.where(inside, parts[g][:, part_at], -jnp.inf), axis=1, keepdims=True
                )
                core = other if k else my_core
                turned = jnp.where(lane == column(mate(k), my_z, core) + t, best, turned)
        turned_rows[z] = turned
        for core in range(CORES):
            if own:
                when(core != my_core, lambda: give_back(z, core).start())
            else:
                give_back(z, core).start()

    def seats(g):
        for s in range(2 * segments):
            k, t = g * 2 * segments // seats_of + s // seats_of, s % seats_of
            if k < plane and t < n:
                v = place_lane[:, :LANES] - s % segments * STEP
                part_at = slice(s // segments * LANES, (s // segments + 1) * LANES)
                yield k, t, part_at, (v >= 0) & (v < STEP)

    def one_by_one(i, carry):
        up = jnp.where(i == 0, my_z - 1, my_z + 1 + i)
        z = jnp.where(my_z == 0, i + 1, jnp.where(my_z > 1, up, my_z + 2 + i))
        compare(z, "above", i == hosted - 1)
        return carry

    late_own = (my_z == 0) & (my_xy > 0)
    when(~late_own, lambda: compare(my_z, "own"))
    lax.fori_loop(0, hosted, one_by_one, 0)
    when(late_own, lambda: compare(my_z, "own"))
    when(at_origin, lambda: compare(deep, "corner"))

    total[...] = turned_rows[my_z]

    def collect(z, core):
        pltpu.make_async_remote_copy(
            src_ref=turned_rows.at[0],
            dst_ref=from_column.at[z, core],
            send_sem=turned_sem.at[z * CORES + core],
            recv_sem=from_column_sem.at[z * CORES + core],
            device_id=place(my_xy, my_z, other),
            device_id_type=MESH,
        ).wait_recv()
        total[...] += from_column[z, core]

    for z in range(deep):
        for core in range(CORES):
            when(
                compared(my_z, z) | ((z == my_z) & (core != my_core)),
                lambda: collect(z, core),
            )
    total[...] = pltpu.roll(total[...], (SUBS - my_core * n) % SUBS, 0)
    total[...] += answers[0]

    def hear(xy):
        pltpu.make_async_remote_copy(
            src_ref=answers.at[0],
            dst_ref=from_plane.at[xy],
            send_sem=answer_sem.at[0],
            recv_sem=from_plane_sem.at[xy],
            device_id=place(xy, my_z, other),
            device_id_type=MESH,
        ).wait_recv()
        total[...] += from_plane[xy]

    when(hosted > 0, lambda: mates(hear))
    out_ref[...] = total[:n, : out_ref.shape[1]]

    for z in range(1, deep):
        when(compared(my_z, z), lambda: gone(z))
    to_column(my_z, other).wait_send()
    mates(lambda xy: to_mate(xy).wait_send())
    when(hosted > 0, lambda: each(plane - 1, lambda k: answer(k + 1).wait_send()))
    for z in range(1, deep):
        for core in range(CORES):
            when(compared(z, my_z), lambda: give_back(z, core).wait_send())
    give_back(my_z, other).wait_send()
    for core in range(CORES):
        when(at_corner, lambda: to_origin(core).wait_send())
    when(at_foot, lambda: hand_over().wait_send())


def body(templates):
    n, comps, samples = templates.shape
    rows = lax.axis_size("row")
    cols = lax.axis_size("col")
    chunks = samples // LANES
    series = n * comps
    lines = series * chunks
    wide = 2 ** int(math.log2(math.sqrt(cols)))
    deep = cols // wide
    plane = rows // CORES * wide
    out_width = rows * cols * n
    width = out_width + -out_width % LANES
    tiles = chunks + 1
    spread = plane * LANES // 2
    spread += -spread % (2 * LANES)
    dma = pltpu.SemaphoreType.DMA
    return pl.pallas_call(
        functools.partial(kernel, rows, cols),
        out_shape=pltpu.VMEM((n, out_width), jnp.float32),
        in_specs=[pl.BlockSpec(memory_space=pltpu.HBM)],
        out_specs=pl.BlockSpec(memory_space=pltpu.VMEM),
        scratch_shapes=[
            pltpu.VMEM(templates.shape, jnp.float32),
            pltpu.VMEM((lines, LANES), jnp.float32),
            pltpu.VMEM((plane, comps, n, chunks, LANES), jnp.bfloat16),
            pltpu.VMEM((deep + 1, CORES, comps, n, chunks, LANES), jnp.bfloat16),
            pltpu.VMEM((plane * lines, LANES), jnp.float32),
            pltpu.VMEM((comps, SUBS * chunks, LANES), jnp.float32),
            pltpu.VMEM(
                (LANES // STEP // 2, comps, 2 * SUBS, samples + 5 * LANES), jnp.bfloat16
            ),
            pltpu.VMEM((comps * samples + LANES, spread), jnp.bfloat16),
            pltpu.VMEM((plane + 1, SUBS, width), jnp.float32),
            pltpu.VMEM((deep, SUBS, width), jnp.float32),
            pltpu.VMEM((plane, SUBS, width), jnp.float32),
            pltpu.VMEM((deep, CORES, SUBS, width), jnp.float32),
            pltpu.VMEM((SUBS, width), jnp.float32),
            dma((plane,)),
            dma(((deep + 1) * CORES,)),
            dma(((deep + 1) * CORES,)),
            dma((plane,)),
            dma((plane,)),
            dma((deep * CORES,)),
            dma((plane,)),
            dma((deep * CORES,)),
            dma((1,)),
            pltpu.SemaphoreType.REGULAR,
            pltpu.SemaphoreType.REGULAR,
        ],
        compiler_params=pltpu.CompilerParams(collective_id=0, has_side_effects=True),
    )(templates)


def solution(mesh):
    placed = (P(("row", "col"), None, None),)
    return jax.shard_map(
        body, mesh=mesh, in_specs=placed, out_specs=P(("row", "col"), None), check_vma=False
    )
```

```python
import functools
import math

import jax
import jax.numpy as jnp
from jax import lax
from jax.experimental import pallas as pl
from jax.experimental.pallas import tpu as pltpu
from jax.sharding import PartitionSpec as P

LAGS = 512
LANES = 128
SUBS = 8
CORES = 2
STEP = 16
MESH = pl.DeviceIdType.MESH


def each(count, step):
    if count <= 16:
        for k in range(count):
            step(k)
    else:
        lax.fori_loop(0, count, lambda k, carry: (step(k), carry)[1], 0)


def when(condition, step):
    pl.when(condition)(step)


def kernel(
    rows,
    cols,
    x_hbm,
    out_ref,
    x_ref,
    stage,
    beside,
    column_blocks,
    lines_ref,
    flat,
    waves,
    shifts,
    answers,
    turned_rows,
    from_plane,
    from_column,
    total,
    block_sem,
    column_send_sem,
    column_sem,
    plane_sem,
    answer_sem,
    turned_sem,
    from_plane_sem,
    from_column_sem,
    table_sem,
    up_sem,
    mate_sem,
):
    n, comps, samples = x_ref.shape
    chunks = samples // LANES
    series = n * comps
    lines = series * chunks
    tall = rows // CORES
    wide = 2 ** int(math.log2(math.sqrt(cols)))
    deep = cols // wide
    plane = tall * wide
    width = total.shape[1]
    blocks = LAGS // STEP
    phases = LANES // STEP
    tiles = chunks + 1
    row = lax.axis_index("row")
    col = lax.axis_index("col")
    my_y, my_core = row // CORES, row % CORES
    my_z, my_x = col // wide, col % wide
    my_xy = my_y * wide + my_x
    other = 1 - my_core

    def place(xy, z, core):
        return (xy // wide) * CORES + core, z * wide + xy % wide

    def column(xy, z, core):
        return (((xy // wide) * CORES + core) * cols + z * wide + xy % wide) * n

    def mate(k):
        if plane & (plane - 1):
            return (my_xy + k) % plane
        found, bit = 0, 1
        while bit < plane:
            found, bit = found + (my_xy // bit + k // bit) % 2 * bit, bit * 2
        return found

    def mates(step):
        each(plane - 1, lambda k: step(mate(k + 1)))

    def compared(z, to):
        return (z > 0) & ((to == 0) | (to == z + 1) | ((to > 0) & (to < z - 1)))

    hosted = jnp.where(
        my_z == 0,
        deep - 1,
        jnp.where(my_z > 1, 1, 0) + jnp.maximum(deep - 2 - my_z, 0),
    )

    def above(step):
        for z in range(1, deep):
            for core in range(CORES):
                when(z > my_z, lambda: step(z, core))

    corner = plane - 1, deep - 1
    at_origin = (my_xy == 0) & (my_z == 0)
    at_corner = (my_xy == corner[0]) & (my_z == corner[1])
    at_foot = (my_xy == corner[0]) & (my_z == 0)

    barrier = pltpu.get_barrier_semaphore()

    def greet(xy, z, core):
        pl.semaphore_signal(barrier, inc=1, device_id=place(xy, z, core), device_id_type=MESH)

    def announce(z, core):
        pl.semaphore_signal(
            up_sem, inc=1, device_id=place(my_xy, z, core), device_id_type=MESH
        )

    taken = pltpu.make_async_copy(x_hbm, x_ref, table_sem.at[0])
    taken.start()
    hub = plane - 1
    at_hub = my_xy == hub
    for core in range(CORES):
        when((my_z > 0) & ~at_hub, lambda: greet(hub, my_z, core))
    when(my_z == 0, lambda: mates(lambda xy: greet(xy, my_z, other)))
    above(lambda z, core: greet(my_xy, z, core))
    greet(my_xy, my_z, other)
    for core in range(CORES):
        when(at_origin, lambda: greet(*corner, core))
    waited = CORES * my_z + 1 + jnp.where(at_hub, CORES * (plane - 1), 0)
    waited = waited + jnp.where(at_corner, CORES, 0)
    when(my_z > 0, lambda: pl.semaphore_wait(barrier, waited))

    def admit(xy):
        pl.semaphore_signal(
            mate_sem, inc=1, device_id=place(xy, my_z, other), device_id_type=MESH
        )

    when((my_z > 0) & at_hub, lambda: mates(admit))
    for z in range(1, deep - 1):
        for core in range(CORES):
            when(my_z == z + 1, lambda: announce(z, core))
    taken.wait()

    for t in range(n):
        x = x_ref[t]
        scale = lax.rsqrt(jnp.mean(x * x, axis=1, keepdims=True) + 1e-06) / math.sqrt(samples)
        rounded = (x * scale).astype(jnp.bfloat16).astype(jnp.float32)
        for q in range(chunks):
            stage[pl.ds(t * chunks + q, comps, stride=n * chunks), :] = rounded[
                :, q * LANES : (q + 1) * LANES
            ]
    column_blocks[my_z, my_core] = (
        stage[...].reshape(comps, n, chunks, LANES).astype(jnp.bfloat16)
    )

    when(my_z == 0, lambda: pl.semaphore_wait(barrier, plane))

    mine = column_blocks.at[my_z, my_core]

    def to_column(z, core):
        return pltpu.make_async_remote_copy(
            src_ref=mine,
            dst_ref=mine,
            send_sem=column_send_sem.at[z * CORES + core],
            recv_sem=column_sem.at[my_z * CORES + my_core],
            device_id=place(my_xy, z, core),
            device_id_type=MESH,
        )

    def to_origin(core):
        return pltpu.make_async_remote_copy(
            src_ref=mine,
            dst_ref=column_blocks.at[deep, my_core],
            send_sem=column_send_sem.at[deep * CORES + core],
            recv_sem=column_sem.at[deep * CORES + my_core],
            device_id=place(0, 0, core),
            device_id_type=MESH,
        )

    def to_mate(xy):
        return pltpu.make_async_remote_copy(
            src_ref=mine,
            dst_ref=beside.at[my_xy],
            send_sem=block_sem.at[xy],
            recv_sem=plane_sem.at[my_xy],
            device_id=place(xy, my_z, other),
            device_id_type=MESH,
        )

    def from_above(z, core):
        block = column_blocks.at[z, core]
        return pltpu.make_async_remote_copy(
            src_ref=block,
            dst_ref=block,
            send_sem=column_send_sem.at[core],
            recv_sem=column_sem.at[z * CORES + core],
            device_id=place(my_xy, my_z, other),
            device_id_type=MESH,
        )

    def hand_over():
        block = column_blocks.at[deep - 1, other]
        return pltpu.make_async_remote_copy(
            src_ref=block,
            dst_ref=block,
            send_sem=column_send_sem.at[(deep - 1) * CORES],
            recv_sem=column_sem.at[(deep - 1) * CORES + other],
            device_id=place(my_xy, my_z, other),
            device_id_type=MESH,
        )

    def from_mate(xy):
        return pltpu.make_async_remote_copy(
            src_ref=mine,
            dst_ref=beside.at[xy],
            send_sem=block_sem.at[xy],
            recv_sem=plane_sem.at[xy],
            device_id=place(xy, my_z, other),
            device_id_type=MESH,
        )

    def send_to(z):
        if z == 0:
            when(~at_corner, lambda: to_column(z, my_core).start())
        else:
            to_column(z, my_core).start()
        to_column(z, other).start()

    when(my_z > 0, lambda: send_to(0))
    for core in range(CORES):
        when(at_corner, lambda: to_origin(core).start())
    to_column(my_z, other).start()
    when((my_z > 0) & ~at_hub, lambda: pl.semaphore_wait(mate_sem, 1))
    mates(lambda xy: to_mate(xy).start())
    def gone(z):
        if z == 0:
            when(~at_corner, lambda: to_column(z, my_core).wait_send())
        else:
            to_column(z, my_core).wait_send()
        to_column(z, other).wait_send()


    for m in range(phases // 2):
        for c in range(comps):
            waves[m, c, :, :LANES] = jnp.zeros((2 * SUBS, LANES), jnp.bfloat16)
            waves[m, c, :, (chunks + 2) * LANES :] = jnp.zeros(
                (2 * SUBS, 3 * LANES), jnp.bfloat16
            )
    answers[...] = jnp.zeros(answers.shape, jnp.float32)

    def settle(k):
        if k == 0:
            block = stage[...]
        else:
            from_mate(mate(k)).wait_recv()
            block = beside[mate(k)].astype(jnp.float32).reshape(lines, LANES)
        lines_ref[k * lines : (k + 1) * lines, :] = block

    segments = LANES // STEP
    seats_of = segments // 2

    room = 2 * STEP

    def stand(g):
        held = range(2 * g, min(2 * g + 2, plane))
        for k in held:
            settle(k)
        local = jnp.concatenate(
            [
                lines_ref[pl.ds(2 * g * lines + q, len(held) * series, stride=chunks), :]
                for q in range(chunks)
            ]
            + [jnp.zeros((len(held) * series, LANES), jnp.float32)],
            axis=1,
        )
        for c in range(comps):
            parts = []
            for s in range(segments):
                k, t = s // seats_of, s % seats_of
                if k < len(held) and t < n:
                    r = k * series + c * n + t
                    line = jnp.broadcast_to(local[r : r + 1], (STEP, tiles * LANES))
                    line = pltpu.roll(line, 0, 1, stride=1, stride_axis=0)
                else:
                    line = jnp.zeros((STEP, tiles * LANES), jnp.float32)
                parts.append(line.astype(jnp.bfloat16))
            stood = jnp.concatenate(parts, axis=0).T
            at = slice(g * LANES, (g + 1) * LANES)
            shifts[c * samples : (c + 1) * samples, at] = stood[:samples]
            tail = comps * samples + c * room
            shifts[tail : tail + room, at] = stood[samples : samples + room]
        unused = comps * samples + comps * room
        shifts[unused:, g * LANES : (g + 1) * LANES] = jnp.zeros(
            (shifts.shape[0] - unused, LANES), jnp.bfloat16
        )

    when(my_z > 0, lambda: gone(0))
    for z in range(1, deep - 2):
        when(my_z > z + 1, lambda: send_to(z))
    when((my_z > 0) & (my_z < deep - 1), lambda: pl.semaphore_wait(up_sem, CORES))
    for z in range(2, deep):
        when(my_z == z - 1, lambda: send_to(z))
    for g in range((plane + 1) // 2):
        stand(g)

    def answer(k):
        return pltpu.make_async_remote_copy(
            src_ref=answers.at[k],
            dst_ref=from_plane.at[my_xy],
            send_sem=answer_sem.at[k],
            recv_sem=from_plane_sem.at[my_xy],
            device_id=place(mate(k), my_z, other),
            device_id_type=MESH,
        )

    def give_back(z, core):
        return pltpu.make_async_remote_copy(
            src_ref=turned_rows.at[z],
            dst_ref=from_column.at[my_z, my_core],
            send_sem=turned_sem.at[z * CORES + core],
            recv_sem=from_column_sem.at[my_z * CORES + my_core],
            device_id=place(my_xy, z, core),
            device_id_type=MESH,
        )

    lane = lax.broadcasted_iota(jnp.int32, (SUBS, width), 1)
    tops = lax.broadcasted_iota(jnp.int32, (SUBS, width), 0)
    place_lane = lax.broadcasted_iota(jnp.int32, (SUBS, 2 * LANES), 1)
    seat = place_lane % STEP
    tail_lane = lax.broadcasted_iota(jnp.int32, (2 * SUBS, LANES), 1)

    def compare(z, kind, final=False):
        own, above_me = kind == "own", kind == "above"
        target = jnp.full((SUBS, width), -1, jnp.int32)
        for core in range(CORES):
            here = (tops >= core * n) & (tops < (core + 1) * n)
            seat_of = column(*corner, core) if kind == "corner" else column(my_xy, z, core)
            target = jnp.where(here, seat_of - core * n + tops, target)
        spot = lane == target

        def prepare(c):
            flat[c, : CORES * n * chunks] = (
                column_blocks[z, :, c].astype(jnp.float32).reshape(CORES * n * chunks, LANES)
            )
            wave = jnp.concatenate(
                [flat[c, pl.ds(q, SUBS, stride=chunks), :] for q in range(chunks)]
                + [jnp.zeros((SUBS, LANES), jnp.float32)],
                axis=1,
            )
            for m in range(phases // 2):
                pair = [
                    wave if b == 0 else pltpu.roll(wave, tiles * LANES - b * STEP, 1)
                    for b in (2 * m, 2 * m + 1)
                ]
                pair = jnp.concatenate(pair, axis=0).astype(jnp.bfloat16)
                waves[m, c, :, 2 * LANES : (chunks + 2) * LANES] = pair[:, :samples]
                waves[m, c, :, LANES : 2 * LANES] = pair[:, samples:]

        def lined_up(c, at, size):
            parts = []
            for p in range(0, blocks + 2, 2):
                start = at + p // phases * LANES
                parts.append(waves[p % phases // 2, c, :, start : start + size])
            return jnp.concatenate(parts, axis=0)

        def lined_up_tails():
            parts = []
            for p in range(0, blocks // 2, 2):
                joined = None
                for c in range(comps):
                    turn = p % phases // 2 - c
                    start = samples + (p // phases + turn // (phases // 2)) * LANES
                    piece = waves[turn % (phases // 2), c, :, start : start + LANES]
                    joined = piece if c == 0 else jnp.where(tail_lane < c * room, joined, piece)
                parts.append(joined)
            return jnp.concatenate(parts, axis=0)

        def products(g):
            at = slice(2 * g * LANES, 2 * (g + 1) * LANES)
            found = jnp.dot(
                jnp.concatenate([lined_up(c, 0, samples) for c in range(comps)], axis=1),
                shifts[: comps * samples, at],
                preferred_element_type=jnp.float32,
            )
            middle = blocks // 2 * SUBS
            ends = jnp.dot(
                lined_up_tails(),
                shifts[comps * samples : comps * samples + LANES, at],
                preferred_element_type=jnp.float32,
            )
            return jnp.concatenate([found[:middle] + ends, found[middle:]], axis=0)

        wholes = shifts.shape[1] // (2 * LANES)
        parted = at_foot & (z == deep - 1)
        if above_me:
            for k in range(1, plane):
                when(parted & (mate(k) == 0), lambda: answer(k).start())
        if own:
            from_above(z, other).wait_recv()
        else:
            from_above(z, other).wait_recv()
            if above_me:
                when(parted, lambda: hand_over().start())
            from_above(z, my_core).wait_recv()
        for c in range(comps):
            prepare(c)

        turned = jnp.zeros((SUBS, width), jnp.float32)
        parts = []
        for g in range(wholes):
            found = products(g)

            def part(p):
                return found[p * SUBS : (p + 1) * SUBS]

            middle = part(1)
            for p in range(2, blocks):
                middle = jnp.maximum(middle, part(p))
            plain = jnp.maximum(middle, part(0))
            swapped = jnp.maximum(middle, jnp.where(seat == 0, part(blocks), part(0)))
            parts.append(swapped)
            for k, t, part_at, inside in seats(g):
                if own or (kind == "corner" and k):
                    break
                into = k if kind == "corner" else jnp.where(parted & (mate(k) == 0), plane, k)
                best = jnp.max(
                    jnp.where(inside, plain[:, part_at], -jnp.inf), axis=1, keepdims=True
                )
                answers[into, t : t + 1] += jnp.sum(
                    jnp.where(spot, best, 0.0), axis=0, keepdims=True
                )
        if kind == "corner":
            return
        if above_me:
            for k in range(1, plane):
                when(final & ~(parted & (mate(k) == 0)), lambda: answer(k).start())
        for g in range(wholes):
            for k, t, part_at, inside in seats(g):
                best = jnp.max(
                    jnp.where(inside, parts[g][:, part_at], -jnp.inf), axis=1, keepdims=True
                )
                core = other if k else my_core
                turned = jnp.where(lane == column(mate(k), my_z, core) + t, best, turned)
        turned_rows[z] = turned
        for core in range(CORES):
            if own:
                when(core != my_core, lambda: give_back(z, core).start())
            else:
                give_back(z, core).start()

    def seats(g):
        for s in range(2 * segments):
            k, t = g * 2 * segments // seats_of + s // seats_of, s % seats_of
            if k < plane and t < n:
                v = place_lane[:, :LANES] - s % segments * STEP
                part_at = slice(s // segments * LANES, (s // segments + 1) * LANES)
                yield k, t, part_at, (v >= 0) & (v < STEP)

    def one_by_one(i, carry):
        up = jnp.where(i == 0, my_z - 1, my_z + 1 + i)
        z = jnp.where(my_z == 0, i + 1, jnp.where(my_z > 1, up, my_z + 2 + i))
        compare(z, "above", i == hosted - 1)
        return carry

    late_own = (my_z == 0) & (my_xy > 0)
    when(~late_own, lambda: compare(my_z, "own"))
    lax.fori_loop(0, hosted, one_by_one, 0)
    when(late_own, lambda: compare(my_z, "own"))
    when(at_origin, lambda: compare(deep, "corner"))

    total[...] = turned_rows[my_z]

    def collect(z, core):
        pltpu.make_async_remote_copy(
            src_ref=turned_rows.at[0],
            dst_ref=from_column.at[z, core],
            send_sem=turned_sem.at[z * CORES + core],
            recv_sem=from_column_sem.at[z * CORES + core],
            device_id=place(my_xy, my_z, other),
            device_id_type=MESH,
        ).wait_recv()
        total[...] += from_column[z, core]

    for z in range(deep):
        for core in range(CORES):
            when(
                compared(my_z, z) | ((z == my_z) & (core != my_core)),
                lambda: collect(z, core),
            )
    total[...] = pltpu.roll(total[...], (SUBS - my_core * n) % SUBS, 0)
    total[...] += answers[0]

    def hear(xy):
        pltpu.make_async_remote_copy(
            src_ref=answers.at[0],
            dst_ref=from_plane.at[xy],
            send_sem=answer_sem.at[0],
            recv_sem=from_plane_sem.at[xy],
            device_id=place(xy, my_z, other),
            device_id_type=MESH,
        ).wait_recv()
        total[...] += from_plane[xy]

    when(hosted > 0, lambda: mates(hear))
    out_ref[...] = total[:n, : out_ref.shape[1]]

    for z in range(1, deep):
        when(compared(my_z, z), lambda: gone(z))
    to_column(my_z, other).wait_send()
    mates(lambda xy: to_mate(xy).wait_send())
    when(hosted > 0, lambda: each(plane - 1, lambda k: answer(k + 1).wait_send()))
    for z in range(1, deep):
        for core in range(CORES):
            when(compared(z, my_z), lambda: give_back(z, core).wait_send())
    give_back(my_z, other).wait_send()
    for core in range(CORES):
        when(at_corner, lambda: to_origin(core).wait_send())
    when(at_foot, lambda: hand_over().wait_send())


def body(templates):
    n, comps, samples = templates.shape
    rows = lax.axis_size("row")
    cols = lax.axis_size("col")
    chunks = samples // LANES
    series = n * comps
    lines = series * chunks
    wide = 2 ** int(math.log2(math.sqrt(cols)))
    deep = cols // wide
    plane = rows // CORES * wide
    out_width = rows * cols * n
    width = out_width + -out_width % LANES
    tiles = chunks + 1
    spread = plane * LANES // 2
    spread += -spread % (2 * LANES)
    dma = pltpu.SemaphoreType.DMA
    return pl.pallas_call(
        functools.partial(kernel, rows, cols),
        out_shape=pltpu.VMEM((n, out_width), jnp.float32),
        in_specs=[pl.BlockSpec(memory_space=pltpu.HBM)],
        out_specs=pl.BlockSpec(memory_space=pltpu.VMEM),
        scratch_shapes=[
            pltpu.VMEM(templates.shape, jnp.float32),
            pltpu.VMEM((lines, LANES), jnp.float32),
            pltpu.VMEM((plane, comps, n, chunks, LANES), jnp.bfloat16),
            pltpu.VMEM((deep + 1, CORES, comps, n, chunks, LANES), jnp.bfloat16),
            pltpu.VMEM((plane * lines, LANES), jnp.float32),
            pltpu.VMEM((comps, SUBS * chunks, LANES), jnp.float32),
            pltpu.VMEM(
                (LANES // STEP // 2, comps, 2 * SUBS, samples + 5 * LANES), jnp.bfloat16
            ),
            pltpu.VMEM((comps * samples + LANES, spread), jnp.bfloat16),
            pltpu.VMEM((plane + 1, SUBS, width), jnp.float32),
            pltpu.VMEM((deep, SUBS, width), jnp.float32),
            pltpu.VMEM((plane, SUBS, width), jnp.float32),
            pltpu.VMEM((deep, CORES, SUBS, width), jnp.float32),
            pltpu.VMEM((SUBS, width), jnp.float32),
            dma((plane,)),
            dma(((deep + 1) * CORES,)),
            dma(((deep + 1) * CORES,)),
            dma((plane,)),
            dma((plane,)),
            dma((deep * CORES,)),
            dma((plane,)),
            dma((deep * CORES,)),
            dma((1,)),
            pltpu.SemaphoreType.REGULAR,
            pltpu.SemaphoreType.REGULAR,
        ],
        compiler_params=pltpu.CompilerParams(collective_id=0, has_side_effects=True),
    )(templates)


def solution(mesh):
    placed = (P(("row", "col"), None, None),)
    return jax.shard_map(
        body, mesh=mesh, in_specs=placed, out_specs=P(("row", "col"), None), check_vma=False
    )
```

```python
import functools
import math

import jax
import jax.numpy as jnp
from jax import lax
from jax.experimental import pallas as pl
from jax.experimental.pallas import tpu as pltpu
from jax.sharding import PartitionSpec as P

LAGS = 512
LANES = 128
SUBS = 8
CORES = 2
STEP = 16
MESH = pl.DeviceIdType.MESH


def each(count, step):
    if count <= 16:
        for k in range(count):
            step(k)
    else:
        lax.fori_loop(0, count, lambda k, carry: (step(k), carry)[1], 0)


def when(condition, step):
    pl.when(condition)(step)


def kernel(
    rows,
    cols,
    x_hbm,
    out_ref,
    x_ref,
    stage,
    beside,
    column_blocks,
    lines_ref,
    flat,
    waves,
    shifts,
    answers,
    turned_rows,
    from_plane,
    from_column,
    total,
    block_sem,
    column_send_sem,
    column_sem,
    plane_sem,
    answer_sem,
    turned_sem,
    from_plane_sem,
    from_column_sem,
    table_sem,
    up_sem,
    mate_sem,
):
    n, comps, samples = x_ref.shape
    chunks = samples // LANES
    series = n * comps
    lines = series * chunks
    tall = rows // CORES
    wide = 2 ** int(math.log2(math.sqrt(cols)))
    deep = cols // wide
    plane = tall * wide
    width = total.shape[1]
    blocks = LAGS // STEP
    phases = LANES // STEP
    tiles = chunks + 1
    row = lax.axis_index("row")
    col = lax.axis_index("col")
    my_y, my_core = row // CORES, row % CORES
    my_z, my_x = col // wide, col % wide
    my_xy = my_y * wide + my_x
    other = 1 - my_core

    def place(xy, z, core):
        return (xy // wide) * CORES + core, z * wide + xy % wide

    def column(xy, z, core):
        return (((xy // wide) * CORES + core) * cols + z * wide + xy % wide) * n

    def mate(k):
        if plane & (plane - 1):
            return (my_xy + k) % plane
        found, bit = 0, 1
        while bit < plane:
            found, bit = found + (my_xy // bit + k // bit) % 2 * bit, bit * 2
        return found

    def mates(step):
        each(plane - 1, lambda k: step(mate(k + 1)))

    def compared(z, to):
        return (z > 0) & ((to == 0) | (to == z + 1) | ((to > 0) & (to < z - 1)))

    hosted = jnp.where(
        my_z == 0,
        deep - 1,
        jnp.where(my_z > 1, 1, 0) + jnp.maximum(deep - 2 - my_z, 0),
    )

    def above(step):
        for z in range(1, deep):
            for core in range(CORES):
                when(z > my_z, lambda: step(z, core))

    corner = plane - 1, deep - 1
    at_origin = (my_xy == 0) & (my_z == 0)
    at_corner = (my_xy == corner[0]) & (my_z == corner[1])
    at_foot = (my_xy == corner[0]) & (my_z == 0)

    barrier = pltpu.get_barrier_semaphore()

    def greet(xy, z, core):
        pl.semaphore_signal(barrier, inc=1, device_id=place(xy, z, core), device_id_type=MESH)

    def announce(z, core):
        pl.semaphore_signal(
            up_sem, inc=1, device_id=place(my_xy, z, core), device_id_type=MESH
        )

    taken = pltpu.make_async_copy(x_hbm, x_ref, table_sem.at[0])
    taken.start()
    hub = plane - 1
    at_hub = my_xy == hub
    for core in range(CORES):
        when((my_z > 0) & ~at_hub, lambda: greet(hub, my_z, core))
    when(my_z == 0, lambda: mates(lambda xy: greet(xy, my_z, other)))
    above(lambda z, core: greet(my_xy, z, core))
    greet(my_xy, my_z, other)
    for core in range(CORES):
        when(at_origin, lambda: greet(*corner, core))
    waited = CORES * my_z + 1 + jnp.where(at_hub, CORES * (plane - 1), 0)
    waited = waited + jnp.where(at_corner, CORES, 0)
    when(my_z > 0, lambda: pl.semaphore_wait(barrier, waited))

    def admit(xy):
        pl.semaphore_signal(
            mate_sem, inc=1, device_id=place(xy, my_z, other), device_id_type=MESH
        )

    when((my_z > 0) & at_hub, lambda: mates(admit))
    for z in range(1, deep - 1):
        for core in range(CORES):
            when(my_z == z + 1, lambda: announce(z, core))
    taken.wait()

    for t in range(n):
        x = x_ref[t]
        scale = lax.rsqrt(jnp.mean(x * x, axis=1, keepdims=True) + 1e-06) / math.sqrt(samples)
        rounded = (x * scale).astype(jnp.bfloat16).astype(jnp.float32)
        for q in range(chunks):
            stage[pl.ds(t * chunks + q, comps, stride=n * chunks), :] = rounded[
                :, q * LANES : (q + 1) * LANES
            ]
    column_blocks[my_z, my_core] = (
        stage[...].reshape(comps, n, chunks, LANES).astype(jnp.bfloat16)
    )

    when(my_z == 0, lambda: pl.semaphore_wait(barrier, plane))

    mine = column_blocks.at[my_z, my_core]

    def to_column(z, core):
        return pltpu.make_async_remote_copy(
            src_ref=mine,
            dst_ref=mine,
            send_sem=column_send_sem.at[z * CORES + core],
            recv_sem=column_sem.at[my_z * CORES + my_core],
            device_id=place(my_xy, z, core),
            device_id_type=MESH,
        )

    def to_origin(core):
        return pltpu.make_async_remote_copy(
            src_ref=mine,
            dst_ref=column_blocks.at[deep, my_core],
            send_sem=column_send_sem.at[deep * CORES + core],
            recv_sem=column_sem.at[deep * CORES + my_core],
            device_id=place(0, 0, core),
            device_id_type=MESH,
        )

    def to_mate(xy):
        return pltpu.make_async_remote_copy(
            src_ref=mine,
            dst_ref=beside.at[my_xy],
            send_sem=block_sem.at[xy],
            recv_sem=plane_sem.at[my_xy],
            device_id=place(xy, my_z, other),
            device_id_type=MESH,
        )

    def from_above(z, core):
        block = column_blocks.at[z, core]
        return pltpu.make_async_remote_copy(
            src_ref=block,
            dst_ref=block,
            send_sem=column_send_sem.at[core],
            recv_sem=column_sem.at[z * CORES + core],
            device_id=place(my_xy, my_z, other),
            device_id_type=MESH,
        )

    def hand_over():
        block = column_blocks.at[deep - 1, other]
        return pltpu.make_async_remote_copy(
            src_ref=block,
            dst_ref=block,
            send_sem=column_send_sem.at[(deep - 1) * CORES],
            recv_sem=column_sem.at[(deep - 1) * CORES + other],
            device_id=place(my_xy, my_z, other),
            device_id_type=MESH,
        )

    def from_mate(xy):
        return pltpu.make_async_remote_copy(
            src_ref=mine,
            dst_ref=beside.at[xy],
            send_sem=block_sem.at[xy],
            recv_sem=plane_sem.at[xy],
            device_id=place(xy, my_z, other),
            device_id_type=MESH,
        )

    def send_to(z):
        if z == 0:
            when(~at_corner, lambda: to_column(z, my_core).start())
        else:
            to_column(z, my_core).start()
        to_column(z, other).start()

    when(my_z > 0, lambda: send_to(0))
    for core in range(CORES):
        when(at_corner, lambda: to_origin(core).start())
    to_column(my_z, other).start()
    when((my_z > 0) & ~at_hub, lambda: pl.semaphore_wait(mate_sem, 1))
    mates(lambda xy: to_mate(xy).start())
    def gone(z):
        if z == 0:
            when(~at_corner, lambda: to_column(z, my_core).wait_send())
        else:
            to_column(z, my_core).wait_send()
        to_column(z, other).wait_send()


    for m in range(phases // 2):
        for c in range(comps):
            waves[m, c, :, :LANES] = jnp.zeros((2 * SUBS, LANES), jnp.bfloat16)
            waves[m, c, :, (chunks + 2) * LANES :] = jnp.zeros(
                (2 * SUBS, 3 * LANES), jnp.bfloat16
            )
    answers[...] = jnp.zeros(answers.shape, jnp.float32)

    def settle(k):
        if k == 0:
            block = stage[...]
        else:
            from_mate(mate(k)).wait_recv()
            block = beside[mate(k)].astype(jnp.float32).reshape(lines, LANES)
        lines_ref[k * lines : (k + 1) * lines, :] = block

    segments = LANES // STEP
    seats_of = segments // 2

    room = 2 * STEP

    def stand(g):
        held = range(2 * g, min(2 * g + 2, plane))
        for k in held:
            settle(k)
        local = jnp.concatenate(
            [
                lines_ref[pl.ds(2 * g * lines + q, len(held) * series, stride=chunks), :]
                for q in range(chunks)
            ]
            + [jnp.zeros((len(held) * series, LANES), jnp.float32)],
            axis=1,
        )
        for c in range(comps):
            parts = []
            for s in range(segments):
                k, t = s // seats_of, s % seats_of
                if k < len(held) and t < n:
                    r = k * series + c * n + t
                    line = jnp.broadcast_to(local[r : r + 1], (STEP, tiles * LANES))
                    line = pltpu.roll(line, 0, 1, stride=1, stride_axis=0)
                else:
                    line = jnp.zeros((STEP, tiles * LANES), jnp.float32)
                parts.append(line.astype(jnp.bfloat16))
            stood = jnp.concatenate(parts, axis=0).T
            at = slice(g * LANES, (g + 1) * LANES)
            shifts[c * samples : (c + 1) * samples, at] = stood[:samples]
            tail = comps * samples + c * room
            shifts[tail : tail + room, at] = stood[samples : samples + room]
        unused = comps * samples + comps * room
        shifts[unused:, g * LANES : (g + 1) * LANES] = jnp.zeros(
            (shifts.shape[0] - unused, LANES), jnp.bfloat16
        )

    when(my_z > 0, lambda: gone(0))
    for z in range(1, deep - 2):
        when(my_z > z + 1, lambda: send_to(z))
    when((my_z > 0) & (my_z < deep - 1), lambda: pl.semaphore_wait(up_sem, CORES))
    for z in range(2, deep):
        when(my_z == z - 1, lambda: send_to(z))
    for g in range((plane + 1) // 2):
        stand(g)

    def answer(k):
        return pltpu.make_async_remote_copy(
            src_ref=answers.at[k],
            dst_ref=from_plane.at[my_xy],
            send_sem=answer_sem.at[k],
            recv_sem=from_plane_sem.at[my_xy],
            device_id=place(mate(k), my_z, other),
            device_id_type=MESH,
        )

    def give_back(z, core):
        return pltpu.make_async_remote_copy(
            src_ref=turned_rows.at[z],
            dst_ref=from_column.at[my_z, my_core],
            send_sem=turned_sem.at[z * CORES + core],
            recv_sem=from_column_sem.at[my_z * CORES + my_core],
            device_id=place(my_xy, z, core),
            device_id_type=MESH,
        )

    lane = lax.broadcasted_iota(jnp.int32, (SUBS, width), 1)
    tops = lax.broadcasted_iota(jnp.int32, (SUBS, width), 0)
    place_lane = lax.broadcasted_iota(jnp.int32, (SUBS, 2 * LANES), 1)
    seat = place_lane % STEP
    tail_lane = lax.broadcasted_iota(jnp.int32, (2 * SUBS, LANES), 1)

    def compare(z, kind, final=False):
        own, above_me = kind == "own", kind == "above"
        target = jnp.full((SUBS, width), -1, jnp.int32)
        for core in range(CORES):
            here = (tops >= core * n) & (tops < (core + 1) * n)
            seat_of = column(*corner, core) if kind == "corner" else column(my_xy, z, core)
            target = jnp.where(here, seat_of - core * n + tops, target)
        spot = lane == target

        def prepare(c):
            flat[c, : CORES * n * chunks] = (
                column_blocks[z, :, c].astype(jnp.float32).reshape(CORES * n * chunks, LANES)
            )
            wave = jnp.concatenate(
                [flat[c, pl.ds(q, SUBS, stride=chunks), :] for q in range(chunks)]
                + [jnp.zeros((SUBS, LANES), jnp.float32)],
                axis=1,
            )
            for m in range(phases // 2):
                pair = [
                    wave if b == 0 else pltpu.roll(wave, tiles * LANES - b * STEP, 1)
                    for b in (2 * m, 2 * m + 1)
                ]
                pair = jnp.concatenate(pair, axis=0).astype(jnp.bfloat16)
                waves[m, c, :, 2 * LANES : (chunks + 2) * LANES] = pair[:, :samples]
                waves[m, c, :, LANES : 2 * LANES] = pair[:, samples:]

        def lined_up(c, at, size):
            parts = []
            for p in range(0, blocks if kind == "corner" else blocks + 2, 2):
                start = at + p // phases * LANES
                parts.append(waves[p % phases // 2, c, :, start : start + size])
            return jnp.concatenate(parts, axis=0)

        def lined_up_tails():
            parts = []
            for p in range(0, blocks // 2, 2):
                joined = None
                for c in range(comps):
                    turn = p % phases // 2 - c
                    start = samples + (p // phases + turn // (phases // 2)) * LANES
                    piece = waves[turn % (phases // 2), c, :, start : start + LANES]
                    joined = piece if c == 0 else jnp.where(tail_lane < c * room, joined, piece)
                parts.append(joined)
            return jnp.concatenate(parts, axis=0)

        def products(g):
            at = slice(2 * g * LANES, 2 * (g + 1) * LANES)
            found = jnp.dot(
                jnp.concatenate([lined_up(c, 0, samples) for c in range(comps)], axis=1),
                shifts[: comps * samples, at],
                preferred_element_type=jnp.float32,
            )
            middle = blocks // 2 * SUBS
            ends = jnp.dot(
                lined_up_tails(),
                shifts[comps * samples : comps * samples + LANES, at],
                preferred_element_type=jnp.float32,
            )
            return jnp.concatenate([found[:middle] + ends, found[middle:]], axis=0)

        wholes = shifts.shape[1] // (2 * LANES)
        parted = at_foot & (z == deep - 1)
        if above_me:
            for k in range(1, plane):
                when(parted & (mate(k) == 0), lambda: answer(k).start())
        if own:
            from_above(z, other).wait_recv()
        else:
            from_above(z, other).wait_recv()
            if above_me:
                when(parted, lambda: hand_over().start())
            from_above(z, my_core).wait_recv()
        for c in range(comps):
            prepare(c)

        turned = jnp.zeros((SUBS, width), jnp.float32)
        parts = []
        for g in range(wholes):
            found = products(g)

            def part(p):
                return found[p * SUBS : (p + 1) * SUBS]

            middle = part(1)
            for p in range(2, blocks):
                middle = jnp.maximum(middle, part(p))
            plain = jnp.maximum(middle, part(0))
            if kind != "corner":
                parts.append(
                    jnp.maximum(middle, jnp.where(seat == 0, part(blocks), part(0)))
                )
            for k, t, part_at, inside in seats(g):
                if own or (kind == "corner" and k):
                    break
                into = k if kind == "corner" else jnp.where(parted & (mate(k) == 0), plane, k)
                best = jnp.max(
                    jnp.where(inside, plain[:, part_at], -jnp.inf), axis=1, keepdims=True
                )
                answers[into, t : t + 1] += jnp.sum(
                    jnp.where(spot, best, 0.0), axis=0, keepdims=True
                )
        if kind == "corner":
            return
        if above_me:
            for k in range(1, plane):
                when(final & ~(parted & (mate(k) == 0)), lambda: answer(k).start())
        for g in range(wholes):
            for k, t, part_at, inside in seats(g):
                best = jnp.max(
                    jnp.where(inside, parts[g][:, part_at], -jnp.inf), axis=1, keepdims=True
                )
                core = other if k else my_core
                turned = jnp.where(lane == column(mate(k), my_z, core) + t, best, turned)
        turned_rows[z] = turned
        for core in range(CORES):
            if own:
                when(core != my_core, lambda: give_back(z, core).start())
            else:
                give_back(z, core).start()

    def seats(g):
        for s in range(2 * segments):
            k, t = g * 2 * segments // seats_of + s // seats_of, s % seats_of
            if k < plane and t < n:
                v = place_lane[:, :LANES] - s % segments * STEP
                part_at = slice(s // segments * LANES, (s // segments + 1) * LANES)
                yield k, t, part_at, (v >= 0) & (v < STEP)

    def one_by_one(i, carry):
        up = jnp.where(i == 0, my_z - 1, my_z + 1 + i)
        z = jnp.where(my_z == 0, i + 1, jnp.where(my_z > 1, up, my_z + 2 + i))
        compare(z, "above", i == hosted - 1)
        return carry

    late_own = (my_z == 0) & (my_xy > 0)
    when(~late_own, lambda: compare(my_z, "own"))
    lax.fori_loop(0, hosted, one_by_one, 0)
    when(late_own, lambda: compare(my_z, "own"))
    when(at_origin, lambda: compare(deep, "corner"))

    total[...] = turned_rows[my_z]

    def collect(z, core):
        pltpu.make_async_remote_copy(
            src_ref=turned_rows.at[0],
            dst_ref=from_column.at[z, core],
            send_sem=turned_sem.at[z * CORES + core],
            recv_sem=from_column_sem.at[z * CORES + core],
            device_id=place(my_xy, my_z, other),
            device_id_type=MESH,
        ).wait_recv()
        total[...] += from_column[z, core]

    for z in range(deep):
        for core in range(CORES):
            when(
                compared(my_z, z) | ((z == my_z) & (core != my_core)),
                lambda: collect(z, core),
            )
    total[...] = pltpu.roll(total[...], (SUBS - my_core * n) % SUBS, 0)
    total[...] += answers[0]

    def hear(xy):
        pltpu.make_async_remote_copy(
            src_ref=answers.at[0],
            dst_ref=from_plane.at[xy],
            send_sem=answer_sem.at[0],
            recv_sem=from_plane_sem.at[xy],
            device_id=place(xy, my_z, other),
            device_id_type=MESH,
        ).wait_recv()
        total[...] += from_plane[xy]

    when(hosted > 0, lambda: mates(hear))
    out_ref[...] = total[:n, : out_ref.shape[1]]

    for z in range(1, deep):
        when(compared(my_z, z), lambda: gone(z))
    to_column(my_z, other).wait_send()
    mates(lambda xy: to_mate(xy).wait_send())
    when(hosted > 0, lambda: each(plane - 1, lambda k: answer(k + 1).wait_send()))
    for z in range(1, deep):
        for core in range(CORES):
            when(compared(z, my_z), lambda: give_back(z, core).wait_send())
    give_back(my_z, other).wait_send()
    for core in range(CORES):
        when(at_corner, lambda: to_origin(core).wait_send())
    when(at_foot, lambda: hand_over().wait_send())


def body(templates):
    n, comps, samples = templates.shape
    rows = lax.axis_size("row")
    cols = lax.axis_size("col")
    chunks = samples // LANES
    series = n * comps
    lines = series * chunks
    wide = 2 ** int(math.log2(math.sqrt(cols)))
    deep = cols // wide
    plane = rows // CORES * wide
    out_width = rows * cols * n
    width = out_width + -out_width % LANES
    tiles = chunks + 1
    spread = plane * LANES // 2
    spread += -spread % (2 * LANES)
    dma = pltpu.SemaphoreType.DMA
    return pl.pallas_call(
        functools.partial(kernel, rows, cols),
        out_shape=pltpu.VMEM((n, out_width), jnp.float32),
        in_specs=[pl.BlockSpec(memory_space=pltpu.HBM)],
        out_specs=pl.BlockSpec(memory_space=pltpu.VMEM),
        scratch_shapes=[
            pltpu.VMEM(templates.shape, jnp.float32),
            pltpu.VMEM((lines, LANES), jnp.float32),
            pltpu.VMEM((plane, comps, n, chunks, LANES), jnp.bfloat16),
            pltpu.VMEM((deep + 1, CORES, comps, n, chunks, LANES), jnp.bfloat16),
            pltpu.VMEM((plane * lines, LANES), jnp.float32),
            pltpu.VMEM((comps, SUBS * chunks, LANES), jnp.float32),
            pltpu.VMEM(
                (LANES // STEP // 2, comps, 2 * SUBS, samples + 5 * LANES), jnp.bfloat16
            ),
            pltpu.VMEM((comps * samples + LANES, spread), jnp.bfloat16),
            pltpu.VMEM((plane + 1, SUBS, width), jnp.float32),
            pltpu.VMEM((deep, SUBS, width), jnp.float32),
            pltpu.VMEM((plane, SUBS, width), jnp.float32),
            pltpu.VMEM((deep, CORES, SUBS, width), jnp.float32),
            pltpu.VMEM((SUBS, width), jnp.float32),
            dma((plane,)),
            dma(((deep + 1) * CORES,)),
            dma(((deep + 1) * CORES,)),
            dma((plane,)),
            dma((plane,)),
            dma((deep * CORES,)),
            dma((plane,)),
            dma((deep * CORES,)),
            dma((1,)),
            pltpu.SemaphoreType.REGULAR,
            pltpu.SemaphoreType.REGULAR,
        ],
        compiler_params=pltpu.CompilerParams(collective_id=0, has_side_effects=True),
    )(templates)


def solution(mesh):
    placed = (P(("row", "col"), None, None),)
    return jax.shard_map(
        body, mesh=mesh, in_specs=placed, out_specs=P(("row", "col"), None), check_vma=False
    )
```
